128 devices in a mesh: expert: 16 (over z, x), replica: 8 (over y, core).
Axes of the slice: x: 4, y: 4, z: 4, core: 2. Of those that a mesh axis runs over, the one named last changes fastest.
Arguments:
- mantissa: bfloat16 [4194304, 128], P(('expert', 'replica')), may hold values from -4 to 4
- scales: bfloat16 [4194304], P(('expert', 'replica')), may hold values from 0.25 to 4
- counts: int32 [8192], P(('expert', 'replica')), may hold values from 256 to 512, as said below
- owner_map: int32 [1024], replicated, may hold values from 0 to 1023, each once
Outputs:
- out_mantissa: bfloat16 [32768, 128], P(('expert', 'replica'))
- out_scales: float32 [32768], P(('expert', 'replica'))
The draws below stay inside these ranges and needn't reach their ends.
Inputs may be any that keep to these rules, and one draw needn't show every extreme that they name: A device's live blocks of an expert are that expert's first counts blocks; some expert has 512 live blocks on every device, and some expert has its last block dead on every device. `owner_map`: each of 0 to 1023 appears once.
All inputs are finite; a program needn't handle non-finite values. Where the reference program divides by a largest or mean magnitude, that divisor is 1e-20 or more.
Results may differ from the reference program's by a relative error of at most 0.001.
Values may be sent and summed in bfloat16 or wider, within the bound.
A program may use at most 128 MiB of HBM per device.

```python
import math
import jax
import jax.numpy as jnp
from jax import lax

EXPERTS = 64
BLOCK = 128
GROUP = 32
BLK = 512
SOURCES = 128
NB = 32768


def draw_counts(key, part):
    gap_key = jax.random.fold_in(key, 11)
    chosen_key = jax.random.fold_in(key, 12)
    second_key = jax.random.fold_in(key, 13)
    device_key = jax.random.fold_in(key, 14)
    expert_gaps = jax.random.randint(gap_key, (EXPERTS,), 0, BLK // 2 + 1)
    chosen = jax.random.randint(chosen_key, (), 0, EXPERTS)
    second = (chosen + 1 + jax.random.randint(second_key, (), 0, EXPERTS - 1)) % EXPERTS
    expert_ids = jnp.arange(EXPERTS)
    expert_gaps = jnp.where(expert_ids == chosen, jnp.maximum(expert_gaps, 1), expert_gaps)
    expert_gaps = jnp.where(expert_ids == second, 0, expert_gaps)
    dropped = jax.random.randint(device_key, (SOURCES, EXPERTS), 0, expert_gaps[None, :] + 1)
    dropped = jnp.where((expert_ids == chosen)[None, :], jnp.maximum(dropped, 1), dropped)
    return (BLK - dropped).reshape(SOURCES * EXPERTS).astype(jnp.int32)


def steps_of(own_key, shape, split, smallest, largest):
    loudness, own = 1.0, jax.random.fold_in(own_key, 6)
    for dim, blocks in split:
        draws = jnp.exp(jax.random.uniform(jax.random.fold_in(own, dim), (blocks,), jnp.float32, smallest / len(split), largest / len(split)))
        loudness = loudness * jnp.repeat(draws, shape[dim] // blocks).reshape([-1 if axis == dim else 1 for axis in range(len(shape))])
    return loudness


def noise(stream_key, extent, spread, bound, split=(), kind=jnp.bfloat16):
    loudness = steps_of(stream_key, extent, split, -0.22, 0.18) if split else 1.0
    entries = jax.random.normal(stream_key, extent, jnp.float32) * spread * loudness
    return jnp.minimum(jnp.maximum(entries, -bound), bound).astype(kind)


def setup_inputs(seed: int = 0) -> dict:
    key_of = jax.random.split(jax.random.key(seed), 5)
    return {
        "mantissa": noise(key_of[0], (SOURCES * NB, BLOCK), 1.0, 4.0, ((0, 128),)),
        "scales": jnp.clip(jnp.exp(math.log(4.0) - 2.7725887 * jax.random.uniform(key_of[1], (SOURCES * NB,), jnp.float32) ** steps_of(key_of[1], (SOURCES * NB,), ((0, 128),), -0.2, 0.2)), 0.25, 4.0).astype(jnp.bfloat16),
        "counts": draw_counts(jax.random.fold_in(key_of[4], 71), 0),
        "owner_map": jax.random.permutation(key_of[3], NB // GROUP).astype(jnp.int32),
    }


clip_target = 0.05
epsilon = 1e-06

def reference(mantissa, scales, counts, owner_map):
    mantissas = mantissa.reshape(SOURCES, NB, BLOCK)
    scale_rows = scales.reshape(SOURCES, NB)
    load_rows = counts.reshape(SOURCES, EXPERTS)
    in_expert = (jnp.arange(NB, dtype=jnp.int32) % BLK).astype(jnp.int32)

    def accumulate(state_pair, source_item):
        summed, contributors = state_pair
        piece, source_scale, source_load = source_item
        is_live = jnp.repeat(source_load, BLK) > in_expert
        factor = jnp.where(is_live, source_scale.astype(jnp.float32), jnp.zeros((NB,), jnp.float32))
        summed = summed + piece.astype(jnp.float32) * factor[:, None]
        contributors = contributors + is_live.astype(jnp.int32)
        return ((summed, contributors), None)
    initial = (jnp.zeros((NB, BLOCK), jnp.float32), jnp.zeros((NB,), jnp.int32))
    (summed, contributors), _ = lax.scan(accumulate, initial, (mantissas, scale_rows, load_rows))
    averaged = summed / jnp.maximum(contributors, 1).astype(jnp.float32)[:, None]
    row_ids = (owner_map.astype(jnp.int32)[:, None] * GROUP + jnp.arange(GROUP, dtype=jnp.int32)[None, :]).reshape(NB).astype(jnp.int32)
    averaged = jnp.take(averaged, row_ids, axis=0)
    root_mean = jnp.sqrt(jnp.sum(averaged * averaged) / (NB * BLOCK) + epsilon)
    clip_factor = jnp.minimum(1.0, clip_target / root_mean)
    clipped = averaged * clip_factor
    block_peak = lax.optimization_barrier(jnp.max(jnp.abs(clipped), axis=1)) + epsilon
    return ((clipped / block_peak[:, None]).astype(jnp.bfloat16), block_peak)
```

```python
import jax
import jax.numpy as jnp
from jax import lax
from jax.experimental import pallas as pl
from jax.experimental.pallas import tpu as pltpu
from jax.sharding import PartitionSpec as P

MESH = pl.DeviceIdType.MESH
AXES = ("expert", "replica")
GROUP = 32
CLIP = 0.05
EPS = 1e-06
ROWS = (96, 80, 80)
START = (0, 96, 176)
PIECES = (
    ((0, 0, 32), (1, 0, 32), (2, 0, 32)),
    ((3, 0, 32), (4, 0, 32), (5, 0, 16)),
    ((5, 16, 16), (6, 0, 32), (7, 0, 32)),
)
ORDER = (2, 1, 3, 0)
FAR, OWN, BOTH = 0, 1, 2
TOP = 32767.0
LOADS = 8


def pick(k, a, b, c):
    return a * ((1 - k) * (2 - k) // 2) + b * (k * (2 - k)) + c * (k * (k - 1) // 2)


def kernel(owner, mant_hbm, scale, eye, out, peak, mant, far_scale, fin, red_send, red_recv, *rest):
    rest = list(rest)

    def take(n):
        head = rest[:n]
        del rest[:n]
        return head

    dsend, drecv, own, near = take(3), take(3), take(3), take(3)
    own_n, near_n = take(3), take(3)
    q1, r1, t1, u1 = take(3), take(3), take(3), take(3)
    mid, mid_n = take(3), take(3)
    q2, r2, t2, u2 = take(3), take(3), take(3), take(3)
    q3, r3, t3, u3 = take(3), take(3), take(3), take(3)
    load_sem, pair_sem, fs_sem, sem1, sem2, sem3, red_sem = rest

    e, r = lax.axis_index("expert"), lax.axis_index("replica")
    z, x = lax.div(e, 4), lax.rem(e, 4)
    y, core = lax.div(r, 2), lax.rem(r, 2)
    partner = (e, z * 0 + y * 2 + 1 - core)

    def moved(c, p, ra, rb, rc):
        first = lax.rem(p + c, 3)
        dx, dy, dz = (pick(lax.rem(dim + 3 - first, 3), ra, rb, rc) for dim in range(3))
        return lax.rem(x + dx, 4), lax.rem(y + dy, 4), lax.rem(z + dz, 4)

    def chip_of(c, p, ra, rb, rc):
        x2, y2, z2 = moved(c, p, ra, rb, rc)
        return (z2 * 4 + x2) * 4 + y2

    def peer(p, role, rel):
        rels = [0, 0, 0]
        rels[role] = rel
        x2, y2, z2 = moved(core, p, *rels)
        return (z2 * 4 + x2, y2 * 2 + core)

    def remote(src, dst, sems, device):
        return pltpu.make_async_remote_copy(
            src_ref=src, dst_ref=dst, send_sem=sems.at[0], recv_sem=sems.at[1],
            device_id=device, device_id_type=MESH,
        )

    def load(i):
        part = pl.ds(i * (1024 // LOADS), 1024 // LOADS)
        return pltpu.make_async_copy(mant_hbm.at[part], mant.at[part], load_sem.at[i])

    for i in range(LOADS):
        load(i).start()

    barrier = pltpu.get_barrier_semaphore()
    greeted = [partner]
    for rel in (1, 2, 3):
        greeted += [(z * 4 + lax.rem(x + rel, 4), r), (e, lax.rem(y + rel, 4) * 2 + core),
                    (lax.rem(z + rel, 4) * 4 + x, r)]
    for device in greeted:
        pl.semaphore_signal(barrier, inc=1, device_id=device, device_id_type=MESH)
    pl.semaphore_wait(barrier, len(greeted))

    fs_copy = remote(scale.at[1 - core], far_scale, fs_sem, partner)
    fs_copy.start()
    for i in range(LOADS):
        load(i).wait()

    def pair_copy(p, k):
        return remote(dsend[p].at[k], drecv[p].at[k], pair_sem.at[p, k], partner)

    for k in range(4):
        for p in range(3):

            @pl.loop(0, 4)
            def _(rb, p=p, k=k):
                for rc in range(4):
                    chip = chip_of(1 - core, p, ORDER[k], rb, rc)
                    first = (chip * 2 + 1 - core) * 8
                    at = 0
                    for g, r0, n in PIECES[p]:
                        dsend[p][k, rb * 4 + rc, pl.ds(at, n)] = mant[owner[first + g], pl.ds(r0, n)]
                        at += n

            pair_copy(p, k).start()

    def column(row, n):
        return jnp.sum(row * eye[pl.ds(0, n)], axis=1, keepdims=True)

    def product(p, k, rel, rb, rc):
        n = ROWS[p]
        chip = chip_of(core, p, rel, rb, rc)
        first = (chip * 2 + core) * 8
        mine = jnp.concatenate(
            [mant[owner[first + g], pl.ds(r0, m)].astype(jnp.float32) for g, r0, m in PIECES[p]], axis=0
        )
        other = drecv[p][k, rb * 4 + rc].astype(jnp.float32)
        s1 = scale[core, p, pl.ds(chip, 1)]
        s2 = far_scale[p, pl.ds(chip, 1)]
        count = jnp.where(s1 > 0.0, 1.0, 0.0) + jnp.where(s2 > 0.0, 1.0, 0.0)
        return mine * column(s1, n) + other * column(s2, n), count

    def quantize(v):
        n = v.shape[0]
        most = jnp.maximum(jnp.max(jnp.abs(v), axis=1, keepdims=True), 1e-30)
        q = lax.round(v * (TOP / most), lax.RoundingMethod.TO_NEAREST_EVEN)
        step = jnp.sum((most * (1.0 / TOP)) * eye[pl.ds(0, n)], axis=0, keepdims=True)
        return q.astype(jnp.int32).astype(jnp.int16), step

    def restored(q, row):
        return q.astype(jnp.int32).astype(jnp.float32) * column(row, q.shape[0])

    def copies1(p, d, kind):
        device = peer(p, 0, 1 + 2 * d)
        return (
            remote(q1[p].at[d, kind], r1[p].at[d, kind], sem1.at[p, d, kind, 0], device),
            remote(t1[p].at[d, kind], u1[p].at[d, kind], sem1.at[p, d, kind, 1], device),
        )

    def send1(p, d, kind, values):
        coded = [quantize(v) for v, _ in values]
        for u, ((q, step), (_, count)) in enumerate(zip(coded, values)):
            q1[p][d, kind, u] = q
            t1[p][d, kind, 0, pl.ds(u, 1)] = step
            t1[p][d, kind, 1, pl.ds(u, 1)] = count
        for copy in copies1(p, d, kind):
            copy.start()

    fs_copy.wait_recv()
    for p in range(3):
        pair_copy(p, 0).wait_recv()

        @pl.loop(0, 2)
        def _(d, p=p):
            send1(p, d, FAR, [product(p, 0, 2, d * 2 + u // 4, u % 4) for u in range(8)])

    for p in range(3):
        for d in range(2):
            pair_copy(p, 1 + d).wait_recv()

        @pl.loop(0, 2)
        def _(d, p=p):
            send1(p, d, OWN, [product(p, 1 + d, 1 + 2 * d, (1 - d) * 2 + u // 4, u % 4) for u in range(8)])

    for p in range(3):

        @pl.loop(0, 2)
        def _(d, p=p):
            values = [product(p, 1 + d, 1 + 2 * d, d * 2 + u // 4, u % 4) for u in range(8)]
            for u, (v, count) in enumerate(values):
                near[p][d, u] = v
                near_n[p][d, pl.ds(u, 1)] = count

    for p in range(3):

        @pl.loop(0, 2)
        def _(d, p=p):
            for copy in copies1(p, d, FAR):
                copy.wait_recv()
            values = []
            for u in range(8):
                v = near[p][d, u] + restored(r1[p][d, FAR, u], u1[p][d, FAR, 0, pl.ds(u, 1)])
                values.append((v, near_n[p][d, pl.ds(u, 1)] + u1[p][d, FAR, 1, pl.ds(u, 1)]))
            send1(p, d, BOTH, values)

    for p in range(3):
        pair_copy(p, 3).wait_recv()

        @pl.loop(0, 2)
        def _(h, p=p):
            values = [product(p, 3, 0, h * 2 + u // 4, u % 4) for u in range(8)]
            for u, (v, count) in enumerate(values):
                own[p][h, u] = v
                own_n[p][h, pl.ds(u, 1)] = count

    def copies2(p, k):
        device = peer(p, 1, k)
        return (
            remote(q2[p].at[k - 1], r2[p].at[k - 1], sem2.at[p, k - 1, 0], device),
            remote(t2[p].at[k - 1], u2[p].at[k - 1], sem2.at[p, k - 1, 1], device),
        )

    def copies3(p, k):
        device = peer(p, 2, k)
        return (
            remote(q3[p].at[k - 1], r3[p].at[k - 1], sem3.at[p, k - 1, 0], device),
            remote(t3[p].at[k - 1], u3[p].at[k - 1], sem3.at[p, k - 1, 1], device),
        )

    for p in range(3):
        for d in range(2):
            for kind in (OWN, BOTH):
                for copy in copies1(p, d, kind):
                    copy.wait_recv()
        for rb in ORDER:
            h, values = rb // 2, []
            for rc in range(4):
                u = rb % 2 * 4 + rc
                v, count = own[p][h, u], own_n[p][h, pl.ds(u, 1)]
                for d, kind in ((h, BOTH), (1 - h, OWN)):
                    v = v + restored(r1[p][d, kind, u], u1[p][d, kind, 0, pl.ds(u, 1)])
                    count = count + u1[p][d, kind, 1, pl.ds(u, 1)]
                values.append((v, count))
            if rb:
                for rc, (v, count) in enumerate(values):
                    q2[p][rb - 1, rc], step = quantize(v)
                    t2[p][rb - 1, 0, pl.ds(rc, 1)] = step
                    t2[p][rb - 1, 1, pl.ds(rc, 1)] = count
                for copy in copies2(p, rb):
                    copy.start()
            else:
                for rc, (v, count) in enumerate(values):
                    mid[p][rc] = v
                    mid_n[p][pl.ds(rc, 1)] = count

    last = []
    for p in range(3):
        for k in (1, 3, 2):
            for copy in copies2(p, k):
                copy.wait_recv()
        values = []
        for rc in range(4):
            v, count = mid[p][rc], mid_n[p][pl.ds(rc, 1)]
            for k in range(3):
                v = v + restored(r2[p][k, rc], u2[p][k, 0, pl.ds(rc, 1)])
                count = count + u2[p][k, 1, pl.ds(rc, 1)]
            values.append((v, count))
        for rc in (2, 1, 3):
            v, count = values[rc]
            q3[p][rc - 1], step = quantize(v)
            t3[p][rc - 1, pl.ds(0, 1)] = step
            t3[p][rc - 1, pl.ds(1, 1)] = count
            for copy in copies3(p, rc):
                copy.start()
        mid[p][0] = values[0][0]
        mid_n[p][pl.ds(0, 1)] = values[0][1]

    square = jnp.zeros((8, 128), jnp.float32)
    for p in range(3):
        n = ROWS[p]
        for k in (1, 3, 2):
            for copy in copies3(p, k):
                copy.wait_recv()
        v, count = mid[p][0], mid_n[p][pl.ds(0, 1)]
        for k in range(3):
            v = v + restored(r3[p][k], u3[p][k, pl.ds(0, 1)])
            count = count + u3[p][k, pl.ds(1, 1)]
        mean = v / column(jnp.maximum(count, 1.0), n)
        fin[pl.ds(START[p], n)] = mean
        square = square + jnp.sum((mean * mean).reshape(n // 8, 8, 128), axis=0)
    total = jnp.sum(jnp.sum(square, axis=0, keepdims=True), axis=1, keepdims=True)

    levels = [[partner]] + [greeted[1 + dim :: 3] for dim in range(3)]
    reduce_copies = []
    for level, devices in enumerate(levels):
        red_send[level] = jnp.broadcast_to(total, (8, 128))
        copies = [
            remote(red_send.at[level], red_recv.at[level, k], red_sem.at[level, k], device)
            for k, device in enumerate(devices)
        ]
        for copy in copies:
            copy.start()
        for k, copy in enumerate(copies):
            copy.wait_recv()
            total = total + red_recv[level, k, pl.ds(0, 1), pl.ds(0, 1)]
        reduce_copies += copies

    root = jnp.sqrt(total / (32768 * 128) + EPS)
    factor = jnp.minimum(1.0, CLIP / root)
    for h in range(2):
        clipped = fin[pl.ds(h * 128, 128)] * factor
        top = jnp.max(jnp.abs(clipped), axis=1, keepdims=True) + EPS
        out[pl.ds(h * 128, 128)] = (clipped / top).astype(jnp.bfloat16)
        peak[pl.ds(h, 1)] = jnp.sum(top * eye[...], axis=0, keepdims=True)

    fs_copy.wait_send()
    for p in range(3):
        for k in range(4):
            pair_copy(p, k).wait_send()
        for d in range(2):
            for kind in range(3):
                for copy in copies1(p, d, kind):
                    copy.wait_send()
        for k in (1, 2, 3):
            for copy in copies2(p, k) + copies3(p, k):
                copy.wait_send()
    for copy in reduce_copies:
        copy.wait_send()


def scratch():
    f32, bf16, i16 = jnp.float32, jnp.bfloat16, jnp.int16

    def each(shape, dtype):
        return [pltpu.VMEM(shape(n), dtype) for n in ROWS]

    shapes = [
        pltpu.VMEM((1024, GROUP, 128), bf16),
        pltpu.VMEM((3, 64, 128), f32),
        pltpu.VMEM((256, 128), f32),
        pltpu.VMEM((4, 8, 128), f32),
        pltpu.VMEM((4, 3, 8, 128), f32),
    ]
    shapes += each(lambda n: (4, 16, n, 128), bf16) * 2
    shapes += each(lambda n: (2, 8, n, 128), f32) * 2
    shapes += each(lambda n: (2, 8, 128), f32) * 2
    shapes += each(lambda n: (2, 3, 8, n, 128), i16) * 2
    shapes += each(lambda n: (2, 3, 2, 8, 128), f32) * 2
    shapes += each(lambda n: (4, n, 128), f32)
    shapes += each(lambda n: (8, 128), f32)
    shapes += each(lambda n: (3, 4, n, 128), i16) * 2
    shapes += each(lambda n: (3, 2, 8, 128), f32) * 2
    shapes += each(lambda n: (3, n, 128), i16) * 2
    shapes += each(lambda n: (3, 8, 128), f32) * 2
    dma = pltpu.SemaphoreType.DMA
    shapes += [dma((LOADS,)), dma((3, 4, 2)), dma((2,)), dma((3, 2, 3, 2, 2)), dma((3, 3, 2, 2)),
               dma((3, 3, 2, 2)), dma((4, 3, 2))]
    return shapes


def local(mantissa, scales, counts, owner_map):
    position = jnp.arange(512, dtype=jnp.int32)
    live = counts[:, None] > position[None, :]
    lived = jnp.where(live, scales.reshape(64, 512).astype(jnp.float32), 0.0).reshape(1024, GROUP)
    ordered = jnp.take(lived, owner_map, axis=0).reshape(64, 2, 256).transpose(1, 0, 2)
    scale = jnp.stack(
        [jnp.pad(ordered[:, :, s : s + n], ((0, 0), (0, 0), (0, 128 - n))) for s, n in zip(START, ROWS)], axis=1
    )
    vmem = pl.BlockSpec(memory_space=pltpu.VMEM)
    out, peak = pl.pallas_call(
        kernel,
        out_shape=(jax.ShapeDtypeStruct((256, 128), jnp.bfloat16), jax.ShapeDtypeStruct((2, 128), jnp.float32)),
        in_specs=[pl.BlockSpec(memory_space=pltpu.SMEM), pl.BlockSpec(memory_space=pl.ANY), vmem, vmem],
        out_specs=(vmem, vmem),
        scratch_shapes=scratch(),
        compiler_params=pltpu.CompilerParams(
            collective_id=0, has_side_effects=True, vmem_limit_bytes=60 * 1024 * 1024
        ),
    )(owner_map, mantissa.reshape(1024, GROUP, 128), scale, jnp.eye(128, dtype=jnp.float32))
    return out, peak.reshape(256)


def solution(mesh):
    return jax.shard_map(
        local,
        mesh=mesh,
        in_specs=(P(AXES, None), P(AXES), P(AXES), P()),
        out_specs=(P(AXES, None), P(AXES)),
        check_vma=False,
    )
```

```python
import jax
import jax.numpy as jnp
from jax import lax
from jax.experimental import pallas as pl
from jax.experimental.pallas import tpu as pltpu
from jax.sharding import PartitionSpec as P

MESH = pl.DeviceIdType.MESH
AXES = ("expert", "replica")
GROUP = 32
CLIP = 0.05
EPS = 1e-06
ROWS = (96, 80, 80)
START = (0, 96, 176)
PIECES = (
    ((0, 0, 32), (1, 0, 32), (2, 0, 32)),
    ((3, 0, 32), (4, 0, 32), (5, 0, 16)),
    ((5, 16, 16), (6, 0, 32), (7, 0, 32)),
)
ORDER = (2, 1, 3, 0)
BATCHES = 2
WIDTH = 4 // BATCHES
FAR, OWN, BOTH = 0, 1, 2
TOP = 32767.0
LOADS = 8


def pick(k, a, b, c):
    return a * ((1 - k) * (2 - k) // 2) + b * (k * (2 - k)) + c * (k * (k - 1) // 2)


def kernel(owner, counts, mant_hbm, scales, count_row, avg, total_out, *rest):
    rest = list(rest)

    def take(n):
        head = rest[:n]
        del rest[:n]
        return head

    mant, eye, lived, far_lived, turned, lines, far_lines = take(7)
    tile, tiles, table, times, red_send, red_near, red_far = take(7)
    dsend, drecv, own = take(3), take(3), take(3)
    q1, r1, t1, u1 = take(3), take(3), take(3), take(3)
    mid = take(3)
    q2, r2, t2, u2 = take(3), take(3), take(3), take(3)
    q3, r3, t3, u3 = take(3), take(3), take(3), take(3)
    load_sem, pair_sem, fs_sem, sem1, sem2, sem3, near_sem, far_sem = rest

    e, r = lax.axis_index("expert"), lax.axis_index("replica")
    z, x = lax.div(e, 4), lax.rem(e, 4)
    y, core = lax.div(r, 2), lax.rem(r, 2)
    partner = (e, y * 2 + 1 - core)

    def moved(c, p, ra, rb, rc):
        first = lax.rem(p + c, 3)
        dx, dy, dz = (pick(lax.rem(dim + 3 - first, 3), ra, rb, rc) for dim in range(3))
        return lax.rem(x + dx, 4), lax.rem(y + dy, 4), lax.rem(z + dz, 4)

    def first_group(c, p, ra, rb, rc):
        x2, y2, z2 = moved(c, p, ra, rb, rc)
        return (((z2 * 4 + x2) * 4 + y2) * 2 + c) * 8

    def peer(p, role, rel):
        rels = [0, 0, 0]
        rels[role] = rel
        x2, y2, z2 = moved(core, p, *rels)
        return (z2 * 4 + x2, y2 * 2 + core)

    def remote(src, dst, sems, device):
        return pltpu.make_async_remote_copy(
            src_ref=src, dst_ref=dst, send_sem=sems.at[0], recv_sem=sems.at[1],
            device_id=device, device_id_type=MESH,
        )

    def load(i):
        part = pl.ds(i * (1024 // LOADS), 1024 // LOADS)
        return pltpu.make_async_copy(mant_hbm.at[part], mant.at[part], load_sem.at[i])

    for i in range(LOADS):
        load(i).start()

    near_peers = [(e, lax.rem(r + j, 8)) for j in range(1, 8)]
    far_peers = [(lax.rem(e + j, 16), r) for j in range(1, 16)]
    barrier = pltpu.get_barrier_semaphore()
    for device in near_peers + far_peers:
        pl.semaphore_signal(barrier, inc=1, device_id=device, device_id_type=MESH)

    row16 = lax.broadcasted_iota(jnp.int32, (16, 128), 0)
    lane16 = lax.broadcasted_iota(jnp.int32, (16, 128), 1)
    spot = lane16 + lax.rem(row16, 4) * 128
    which = lax.div(row16, 4)

    @pl.loop(0, 16)
    def _(b):
        bound = jnp.where(which < 2, jnp.where(which == 0, counts[b * 4], counts[b * 4 + 1]),
                          jnp.where(which == 2, counts[b * 4 + 2], counts[b * 4 + 3]))
        rows = pl.ds(pl.multiple_of(b * 16, 16), 16)
        lived[rows] = jnp.where(spot < bound, scales[rows].astype(jnp.float32), 0.0)

    def expand(source, target):
        for q in range(4):
            turned[q] = source[...] if q == 0 else pltpu.roll(source[...], 128 - q * GROUP, 1)

        @pl.loop(0, 32)
        def _(b):
            for i in range(8):
                for q in range(4):
                    target[(b * 8 + i) * 4 + q] = turned[q, pl.ds(b * 8 + i, 1)]

    eye[...] = jnp.where(
        lax.broadcasted_iota(jnp.int32, (128, 128), 0) == lax.broadcasted_iota(jnp.int32, (128, 128), 1), 1.0, 0.0
    )
    row8 = lax.broadcasted_iota(jnp.int32, (8, 128), 0)
    tile[...] = jnp.where(row8 == r, jnp.broadcast_to(count_row[...].astype(jnp.float32), (8, 128)), 0.0)
    pl.semaphore_wait(barrier, 22)

    fs_copy = remote(lived, far_lived, fs_sem, partner)
    fs_copy.start()
    count_near = [remote(tile, tiles.at[j], near_sem.at[0, j], near_peers[j]) for j in range(7)]
    count_far = [remote(table.at[e], table.at[e], far_sem.at[0, j], far_peers[j]) for j in range(15)]
    for copy in count_near:
        copy.start()
    expand(lived, lines)
    for i in range(LOADS):
        load(i).wait()

    def pair_copy(p, k, bat):
        part = pl.ds(bat * WIDTH * 4, WIDTH * 4)
        return remote(dsend[p].at[k, part], drecv[p].at[k, part], pair_sem.at[p, k, bat], partner)

    def gather(bat, k):
        for p in range(3):

            @pl.loop(0, WIDTH)
            def _(w):
                c = bat * WIDTH + w
                rc = 2 - c + pick(lax.div(c, 2), 0, 3, 0) - pick(lax.rem(c, 2) * lax.div(c, 2), 0, 2, 0)
                for rb in range(4):
                    first = first_group(1 - core, p, ORDER[k], rb, rc)
                    at = 0
                    for g, r0, n in PIECES[p]:
                        dsend[p][k, c * 4 + rb, pl.ds(at, n)] = mant[owner[first + g], pl.ds(r0, n)]
                        at += n

            pair_copy(p, k, bat).start()

    def column(row, n):
        return jnp.sum(row * eye[pl.ds(0, n)], axis=1, keepdims=True)

    def product(p, k, rb, c):
        first = first_group(core, p, ORDER[k], rb, ORDER[c])
        values, at = [], 0
        for g, r0, n in PIECES[p]:
            group = owner[first + g]
            chosen = eye[pl.ds(r0, n)]
            s1 = jnp.sum(lines[group] * chosen, axis=1, keepdims=True)
            s2 = jnp.sum(far_lines[group] * chosen, axis=1, keepdims=True)
            mine = mant[group, pl.ds(r0, n)].astype(jnp.float32)
            other = drecv[p][k, c * 4 + rb, pl.ds(at, n)].astype(jnp.float32)
            values.append(mine * s1 + other * s2)
            at += n
        return jnp.concatenate(values, axis=0)

    def quantize(v):
        n = v.shape[0]
        most = jnp.maximum(jnp.max(jnp.abs(v), axis=1, keepdims=True), 1e-30)
        q = lax.round(v * (TOP / most), lax.RoundingMethod.TO_NEAREST_EVEN)
        step = jnp.sum((most * (1.0 / TOP)) * eye[pl.ds(0, n)], axis=0, keepdims=True)
        return q.astype(jnp.int32).astype(jnp.int16), step

    def restored(q, row):
        return q.astype(jnp.int32).astype(jnp.float32) * column(row, q.shape[0])

    def copies1(p, d, kind, bat):
        device = peer(p, 0, 1 + 2 * d)
        part = pl.ds(bat * WIDTH * 2, WIDTH * 2)
        return (
            remote(q1[p].at[d, kind, part], r1[p].at[d, kind, part], sem1.at[p, d, kind, bat, 0], device),
            remote(t1[p].at[d, kind, bat], u1[p].at[d, kind, bat], sem1.at[p, d, kind, bat, 1], device),
        )

    def places(bat):
        return [(c, i) for c in range(bat * WIDTH, (bat + 1) * WIDTH) for i in range(2)]

    def first_dim(bat, kind):
        for p in range(3):
            if kind == FAR:
                pair_copy(p, 0, bat).wait_recv()
            if kind == OWN:
                pair_copy(p, 1, bat).wait_recv()
                pair_copy(p, 2, bat).wait_recv()
            if kind == BOTH:
                for d in range(2):
                    for copy in copies1(p, d, FAR, bat):
                        copy.wait_recv()
            coded = []
            for d in range(2):
                half = 1 - d if kind == OWN else d
                for j, (c, i) in enumerate(places(bat)):
                    v = product(p, 0 if kind == FAR else 1 + d, half * 2 + i, c)
                    if kind == BOTH:
                        v = v + restored(r1[p][d, FAR, c * 2 + i], u1[p][d, FAR, bat, pl.ds(j, 1)])
                    coded.append((d, c * 2 + i, j, quantize(v)))
            for d, u, j, (q, step) in coded:
                q1[p][d, kind, u] = q
                t1[p][d, kind, bat, pl.ds(j, 1)] = step
            for d in range(2):
                for copy in copies1(p, d, kind, bat):
                    copy.start()

    def own_share(bat):
        for p in range(3):
            pair_copy(p, 3, bat).wait_recv()
            for c in range(bat * WIDTH, (bat + 1) * WIDTH):
                values = [product(p, 3, rb, c) for rb in range(4)]
                for rb in range(4):
                    own[p][c * 4 + rb] = values[rb]

    def copies2(p, k, bat):
        device = peer(p, 1, k)
        part = pl.ds(bat * WIDTH, WIDTH)
        return (
            remote(q2[p].at[k - 1, part], r2[p].at[k - 1, part], sem2.at[p, k - 1, bat, 0], device),
            remote(t2[p].at[k - 1, bat], u2[p].at[k - 1, bat], sem2.at[p, k - 1, bat, 1], device),
        )

    def second_dim(bat):
        for p in range(3):
            for d in range(2):
                for kind in (OWN, BOTH):
                    for copy in copies1(p, d, kind, bat):
                        copy.wait_recv()
            for rb in ORDER:
                h, values = rb // 2, []
                for w in range(WIDTH):
                    c = bat * WIDTH + w
                    v = own[p][c * 4 + rb]
                    for d, kind in ((h, BOTH), (1 - h, OWN)):
                        v = v + restored(r1[p][d, kind, c * 2 + rb % 2], u1[p][d, kind, bat, pl.ds(w * 2 + rb % 2, 1)])
                    values.append(v)
                if rb:
                    for w, v in enumerate(values):
                        q2[p][rb - 1, bat * WIDTH + w], t2[p][rb - 1, bat, pl.ds(w, 1)] = quantize(v)
                    for copy in copies2(p, rb, bat):
                        copy.start()
                else:
                    for w, v in enumerate(values):
                        mid[p][bat * WIDTH + w] = v

    def copies3(p, k):
        device = peer(p, 2, k)
        return (
            remote(q3[p].at[k - 1], r3[p].at[k - 1], sem3.at[p, k - 1, 0], device),
            remote(t3[p].at[k - 1], u3[p].at[k - 1], sem3.at[p, k - 1, 1], device),
        )

    def third_dim(bat):
        for p in range(3):
            for k in (1, 3, 2):
                for copy in copies2(p, k, bat):
                    copy.wait_recv()
            values = []
            for w in range(WIDTH):
                c = bat * WIDTH + w
                v = mid[p][c]
                for k in range(3):
                    v = v + restored(r2[p][k, c], u2[p][k, bat, pl.ds(w, 1)])
                values.append(v)
            for w, v in enumerate(values):
                rc = ORDER[bat * WIDTH + w]
                if rc:
                    q3[p][rc - 1], t3[p][rc - 1, pl.ds(0, 1)] = quantize(v)
                    for copy in copies3(p, rc):
                        copy.start()
                else:
                    mid[p][3] = v

    def count_sources():
        for copy in count_far:
            copy.wait_recv()
        loads = table[...].reshape(128, 128).T[:64]
        expert = lax.broadcasted_iota(jnp.int32, (64, 128), 0)
        first = (e * 8 + r) * 8
        found = []
        for g in range(8):
            group = owner[first + g]
            place = lax.broadcasted_iota(jnp.int32, (GROUP, 128), 0) + lax.rem(group, 16) * GROUP
            load_line = jnp.sum(jnp.where(expert == lax.div(group, 16), loads, 0.0), axis=0, keepdims=True)
            live = jnp.where(load_line > place.astype(jnp.float32), 1.0, 0.0)
            found.append(jnp.maximum(jnp.sum(live, axis=1, keepdims=True), 1.0))
        for g in range(8):
            times[pl.ds(g * GROUP, GROUP)] = jnp.broadcast_to(found[g], (GROUP, 128))

    for k in (0, 1, 2):
        gather(0, k)
    fs_copy.wait_recv()
    expand(far_lived, far_lines)
    first_dim(0, FAR)
    for k in (0, 1, 2):
        gather(1, k)
    first_dim(0, OWN)
    mine = tile[...]
    for j, copy in enumerate(count_near):
        copy.wait_recv()
        mine = mine + tiles[j]
    table[e] = mine
    for copy in count_far:
        copy.start()
    first_dim(1, FAR)
    gather(0, 3)
    first_dim(0, BOTH)
    gather(1, 3)
    first_dim(1, OWN)
    own_share(0)
    first_dim(1, BOTH)
    own_share(1)
    second_dim(0)
    second_dim(1)
    count_sources()
    third_dim(0)
    third_dim(1)

    square = jnp.zeros((8, 128), jnp.float32)
    for p in range(3):
        n = ROWS[p]
        for k in (1, 3, 2):
            for copy in copies3(p, k):
                copy.wait_recv()
        v = mid[p][3]
        for k in range(3):
            v = v + restored(r3[p][k], u3[p][k, pl.ds(0, 1)])
        mean = v / times[pl.ds(START[p], n)]
        avg[pl.ds(START[p], n)] = mean
        square = square + jnp.sum((mean * mean).reshape(n // 8, 8, 128), axis=0)

    red_send[0] = square
    red_copies = [remote(red_send.at[0], red_near.at[j], near_sem.at[1, j], near_peers[j]) for j in range(7)]
    for copy in red_copies:
        copy.start()
    for j, copy in enumerate(red_copies):
        copy.wait_recv()
        square = square + red_near[j]
    red_send[1] = square
    red_copies2 = [remote(red_send.at[1], red_far.at[j], far_sem.at[1, j], far_peers[j]) for j in range(15)]
    for copy in red_copies2:
        copy.start()
    for j, copy in enumerate(red_copies2):
        copy.wait_recv()
        square = square + red_far[j]
    total_out[...] = square

    fs_copy.wait_send()
    for copy in count_near + count_far + red_copies + red_copies2:
        copy.wait_send()
    for p in range(3):
        for bat in range(BATCHES):
            for k in range(4):
                pair_copy(p, k, bat).wait_send()
            for d in range(2):
                for kind in range(3):
                    for copy in copies1(p, d, kind, bat):
                        copy.wait_send()
            for k in (1, 2, 3):
                for copy in copies2(p, k, bat):
                    copy.wait_send()
        for k in (1, 2, 3):
            for copy in copies3(p, k):
                copy.wait_send()


def scratch():
    f32, bf16, i16 = jnp.float32, jnp.bfloat16, jnp.int16

    def each(shape, dtype):
        return [pltpu.VMEM(shape(n), dtype) for n in ROWS]

    shapes = [
        pltpu.VMEM((1024, GROUP, 128), bf16),
        pltpu.VMEM((128, 128), f32),
        pltpu.VMEM((256, 128), f32),
        pltpu.VMEM((256, 128), f32),
        pltpu.VMEM((4, 256, 128), f32),
        pltpu.VMEM((1024, 1, 128), f32),
        pltpu.VMEM((1024, 1, 128), f32),
        pltpu.VMEM((8, 128), f32),
        pltpu.VMEM((7, 8, 128), f32),
        pltpu.VMEM((16, 8, 128), f32),
        pltpu.VMEM((256, 128), f32),
        pltpu.VMEM((2, 8, 128), f32),
        pltpu.VMEM((7, 8, 128), f32),
        pltpu.VMEM((15, 8, 128), f32),
    ]
    shapes += each(lambda n: (4, 16, n, 128), bf16) * 2
    shapes += each(lambda n: (16, n, 128), f32)
    shapes += each(lambda n: (2, 3, 8, n, 128), i16) * 2
    shapes += each(lambda n: (2, 3, BATCHES, 8, 128), f32) * 2
    shapes += each(lambda n: (4, n, 128), f32)
    shapes += each(lambda n: (3, 4, n, 128), i16) * 2
    shapes += each(lambda n: (3, BATCHES, 8, 128), f32) * 2
    shapes += each(lambda n: (3, n, 128), i16) * 2
    shapes += each(lambda n: (3, 8, 128), f32) * 2
    dma = pltpu.SemaphoreType.DMA
    shapes += [dma((LOADS,)), dma((3, 4, BATCHES, 2)), dma((2,)), dma((3, 2, 3, BATCHES, 2, 2)),
               dma((3, 3, BATCHES, 2, 2)), dma((3, 3, 2, 2)), dma((2, 7, 2)), dma((2, 15, 2))]
    return shapes


def local(mantissa, scales, counts, owner_map):
    vmem, smem = pl.BlockSpec(memory_space=pltpu.VMEM), pl.BlockSpec(memory_space=pltpu.SMEM)
    averaged, square = pl.pallas_call(
        kernel,
        out_shape=(jax.ShapeDtypeStruct((256, 128), jnp.float32), jax.ShapeDtypeStruct((8, 128), jnp.float32)),
        in_specs=[smem, smem, pl.BlockSpec(memory_space=pl.ANY), vmem, vmem],
        out_specs=(vmem, vmem),
        scratch_shapes=scratch(),
        compiler_params=pltpu.CompilerParams(
            collective_id=0, has_side_effects=True, vmem_limit_bytes=60 * 1024 * 1024
        ),
    )(owner_map, counts, mantissa.reshape(1024, GROUP, 128), scales.reshape(256, 128), jnp.pad(counts, (0, 64)).reshape(1, 128))
    root_mean = jnp.sqrt(jnp.sum(square) / (32768 * 128) + EPS)
    clipped = averaged * jnp.minimum(1.0, CLIP / root_mean)
    top = jnp.max(jnp.abs(clipped), axis=1) + EPS
    return (clipped / top[:, None]).astype(jnp.bfloat16), top


def solution(mesh):
    return jax.shard_map(
        local,
        mesh=mesh,
        in_specs=(P(AXES, None), P(AXES), P(AXES), P()),
        out_specs=(P(AXES, None), P(AXES)),
        check_vma=False,
    )
```

```python
import jax
import jax.numpy as jnp
from jax import lax
from jax.experimental import pallas as pl
from jax.experimental.pallas import tpu as pltpu
from jax.sharding import PartitionSpec as P

MESH = pl.DeviceIdType.MESH
AXES = ("expert", "replica")
GROUP = 32
CLIP = 0.05
EPS = 1e-06
ROWS = (96, 80, 80)
START = (0, 96, 176)
PIECES = (
    ((0, 0, 32), (1, 0, 32), (2, 0, 32)),
    ((3, 0, 32), (4, 0, 32), (5, 0, 16)),
    ((5, 16, 16), (6, 0, 32), (7, 0, 32)),
)
ORDER = (2, 1, 3, 0)
BATCHES = 2
WIDTH = 4 // BATCHES
FAR, OWN, BOTH = 0, 1, 2
TOP = 32767.0
LOADS = 8


def pick(k, a, b, c):
    return a * ((1 - k) * (2 - k) // 2) + b * (k * (2 - k)) + c * (k * (k - 1) // 2)


def kernel(owner, counts, mant_hbm, scales, count_row, out, peak, *rest):
    rest = list(rest)

    def take(n):
        head = rest[:n]
        del rest[:n]
        return head

    mant, eye, lived, far_lived, turned, lines, far_lines = take(7)
    tile, tiles, table, times, red_send, red_near, red_far, avg = take(8)
    dsend, drecv, own = take(3), take(3), take(3)
    q1, r1, t1, u1 = take(3), take(3), take(3), take(3)
    mid = take(3)
    q2, r2, t2, u2 = take(3), take(3), take(3), take(3)
    q3, r3, t3, u3 = take(3), take(3), take(3), take(3)
    load_sem, pair_sem, fs_sem, sem1, sem2, sem3, near_sem, far_sem = rest

    e, r = lax.axis_index("expert"), lax.axis_index("replica")
    z, x = lax.div(e, 4), lax.rem(e, 4)
    y, core = lax.div(r, 2), lax.rem(r, 2)
    partner = (e, y * 2 + 1 - core)

    turns = [[lax.rem(v + rel, 4) for rel in range(4)] for v in (x, y, z)]
    weights = (64, 16, 256)

    def turned_by(c):
        return [
            [pick(lax.rem(dim + c, 3), *(turns[i][rel] * weights[i] for i in range(3))) for rel in range(4)]
            for dim in range(3)
        ]

    mine_at, other_at = turned_by(core), turned_by(1 - core)

    def first_group(c, p, ra, rb, rc):
        at = mine_at if c == 0 else other_at
        own_core = core if c == 0 else 1 - core
        return at[p][ra] + at[(p + 1) % 3][rb] + at[(p + 2) % 3][rc] + own_core * 8

    def peer(p, role, rel):
        dim = lax.rem((p + role) % 3 + core, 3)
        x2, y2, z2 = (
            pick(lax.rem(dim + 3 - i, 3), turns[i][rel], turns[i][0], turns[i][0]) for i in range(3)
        )
        return (z2 * 4 + x2, y2 * 2 + core)

    def remote(src, dst, sems, device):
        return pltpu.make_async_remote_copy(
            src_ref=src, dst_ref=dst, send_sem=sems.at[0], recv_sem=sems.at[1],
            device_id=device, device_id_type=MESH,
        )

    def load(i):
        part = pl.ds(i * (1024 // LOADS), 1024 // LOADS)
        return pltpu.make_async_copy(mant_hbm.at[part], mant.at[part], load_sem.at[i])

    for i in range(LOADS):
        load(i).start()

    near_peers = [(e, lax.rem(r + j, 8)) for j in range(1, 8)]
    far_peers = [(lax.rem(e + j, 16), r) for j in range(1, 16)]
    barrier = pltpu.get_barrier_semaphore()
    for device in near_peers + far_peers:
        pl.semaphore_signal(barrier, inc=1, device_id=device, device_id_type=MESH)

    row16 = lax.broadcasted_iota(jnp.int32, (16, 128), 0)
    lane16 = lax.broadcasted_iota(jnp.int32, (16, 128), 1)
    spot = lane16 + lax.rem(row16, 4) * 128
    which = lax.div(row16, 4)

    @pl.loop(0, 16)
    def _(b):
        bound = jnp.where(which < 2, jnp.where(which == 0, counts[b * 4], counts[b * 4 + 1]),
                          jnp.where(which == 2, counts[b * 4 + 2], counts[b * 4 + 3]))
        rows = pl.ds(pl.multiple_of(b * 16, 16), 16)
        lived[rows] = jnp.where(spot < bound, scales[rows].astype(jnp.float32), 0.0)

    def expand(source, target):
        for q in range(4):
            lanes = source[...] if q == 0 else pltpu.roll(source[...], 128 - q * GROUP, 1)
            turned[q] = jnp.where(lax.broadcasted_iota(jnp.int32, (256, 128), 1) < GROUP, lanes, 0.0)

        @pl.loop(0, 32)
        def _(b):
            for i in range(8):
                for q in range(4):
                    target[(b * 8 + i) * 4 + q] = turned[q, pl.ds(b * 8 + i, 1)]

    eye[...] = jnp.where(
        lax.broadcasted_iota(jnp.int32, (128, 128), 0) == lax.broadcasted_iota(jnp.int32, (128, 128), 1), 1.0, 0.0
    )
    row8 = lax.broadcasted_iota(jnp.int32, (8, 128), 0)
    tile[...] = jnp.zeros((8, 128), jnp.float32)
    tile[:, pl.ds(0, 64)] = jnp.where(row8[:, :64] == r, jnp.broadcast_to(count_row[...].astype(jnp.float32), (8, 64)), 0.0)
    pl.semaphore_wait(barrier, 22)

    fs_copy = remote(lived, far_lived, fs_sem, partner)
    fs_copy.start()
    count_near = [remote(tile, tiles.at[j], near_sem.at[0, j], near_peers[j]) for j in range(7)]
    count_far = [remote(table.at[e], table.at[e], far_sem.at[0, j], far_peers[j]) for j in range(15)]
    for copy in count_near:
        copy.start()
    expand(lived, lines)
    for i in range(LOADS):
        load(i).wait()

    def pair_copy(p, k, bat):
        part = pl.ds(bat * WIDTH * 4, WIDTH * 4)
        return remote(dsend[p].at[k, part], drecv[p].at[k, part], pair_sem.at[p, k, bat], partner)

    def gather(bat, k):
        for p in range(3):
            for c in range(bat * WIDTH, (bat + 1) * WIDTH):
                for rb in range(4):
                    first = first_group(1, p, ORDER[k], rb, ORDER[c])
                    at = 0
                    for g, r0, n in PIECES[p]:
                        dsend[p][k, c * 4 + rb, pl.ds(at, n)] = mant[owner[first + g], pl.ds(r0, n)]
                        at += n
            pair_copy(p, k, bat).start()

    lane = lax.broadcasted_iota(jnp.int32, (1, 128), 1)

    def scale_row(source, groups, p):
        row, at = None, 0
        for group, (_, r0, n) in zip(groups, PIECES[p]):
            piece = source[group]
            if n < GROUP:
                piece = jnp.where(lane < n, piece, 0.0) if r0 == 0 else jnp.where(lane < r0, 0.0, piece)
            if at != r0:
                piece = pltpu.roll(piece, (at - r0) % 128, 1)
            row = piece if row is None else row + piece
            at += n
        return row

    def scaled(row, rows):
        n = rows.shape[0]
        weight = (eye[pl.ds(0, n)] * row).astype(jnp.bfloat16)[:, :n]
        return jnp.dot(weight, rows, preferred_element_type=jnp.float32)

    def product(p, k, rb, c):
        first = first_group(0, p, ORDER[k], rb, ORDER[c])
        groups = [owner[first + g] for g, _, _ in PIECES[p]]
        mine = jnp.concatenate([mant[group, pl.ds(r0, n)] for group, (_, r0, n) in zip(groups, PIECES[p])], axis=0)
        other = drecv[p][k, c * 4 + rb]
        return scaled(scale_row(lines, groups, p), mine) + scaled(scale_row(far_lines, groups, p), other)

    def quantize(v):
        n = v.shape[0]
        most = jnp.maximum(jnp.max(jnp.abs(v), axis=1, keepdims=True), 1e-30)
        step = (most * (1.0045 / TOP)).astype(jnp.bfloat16).astype(jnp.float32)
        q = lax.round(v / step, lax.RoundingMethod.TO_NEAREST_EVEN)
        row = jnp.sum(step * eye[pl.ds(0, n)], axis=0, keepdims=True)
        return q.astype(jnp.int32).astype(jnp.int16), row

    def restored(q, row):
        n = q.shape[0]
        weight = (eye[pl.ds(0, n)] * row).astype(jnp.bfloat16)
        step = jnp.dot(weight, jnp.ones((128, 128), jnp.bfloat16), preferred_element_type=jnp.float32)
        return q.astype(jnp.int32).astype(jnp.float32) * step

    def copies1(p, d, kind, bat):
        device = peer(p, 0, 1 + 2 * d)
        part = pl.ds(bat * WIDTH * 2, WIDTH * 2)
        return (
            remote(q1[p].at[d, kind, part], r1[p].at[d, kind, part], sem1.at[p, d, kind, bat, 0], device),
            remote(t1[p].at[d, kind, bat], u1[p].at[d, kind, bat], sem1.at[p, d, kind, bat, 1], device),
        )

    def places(bat):
        return [(c, i) for c in range(bat * WIDTH, (bat + 1) * WIDTH) for i in range(2)]

    def first_dim(bat, kind):
        for p in range(3):
            if kind == FAR:
                pair_copy(p, 0, bat).wait_recv()
            if kind == OWN:
                pair_copy(p, 1, bat).wait_recv()
                pair_copy(p, 2, bat).wait_recv()
            if kind == BOTH:
                for d in range(2):
                    for copy in copies1(p, d, FAR, bat):
                        copy.wait_recv()
            coded = []
            for d in range(2):
                half = 1 - d if kind == OWN else d
                for j, (c, i) in enumerate(places(bat)):
                    v = product(p, 0 if kind == FAR else 1 + d, half * 2 + i, c)
                    if kind == BOTH:
                        v = v + restored(r1[p][d, FAR, c * 2 + i], u1[p][d, FAR, bat, pl.ds(j, 1)])
                    coded.append((d, c * 2 + i, j, quantize(v)))
            for d, u, j, (q, step) in coded:
                q1[p][d, kind, u] = q
                t1[p][d, kind, bat, pl.ds(j, 1)] = step
            for d in range(2):
                for copy in copies1(p, d, kind, bat):
                    copy.start()

    def own_share(bat):
        for p in range(3):
            pair_copy(p, 3, bat).wait_recv()
            for c in range(bat * WIDTH, (bat + 1) * WIDTH):
                values = [product(p, 3, rb, c) for rb in range(4)]
                for rb in range(4):
                    own[p][c * 4 + rb] = values[rb]

    def copies2(p, k, bat):
        device = peer(p, 1, k)
        part = pl.ds(bat * WIDTH, WIDTH)
        return (
            remote(q2[p].at[k - 1, part], r2[p].at[k - 1, part], sem2.at[p, k - 1, bat, 0], device),
            remote(t2[p].at[k - 1, bat], u2[p].at[k - 1, bat], sem2.at[p, k - 1, bat, 1], device),
        )

    def second_dim(bat):
        for p in range(3):
            for d in range(2):
                for kind in (OWN, BOTH):
                    for copy in copies1(p, d, kind, bat):
                        copy.wait_recv()
            for rb in ORDER:
                h, values = rb // 2, []
                for w in range(WIDTH):
                    c = bat * WIDTH + w
                    v = own[p][c * 4 + rb]
                    for d, kind in ((h, BOTH), (1 - h, OWN)):
                        v = v + restored(r1[p][d, kind, c * 2 + rb % 2], u1[p][d, kind, bat, pl.ds(w * 2 + rb % 2, 1)])
                    values.append(v)
                if rb:
                    for w, v in enumerate(values):
                        q2[p][rb - 1, bat * WIDTH + w], t2[p][rb - 1, bat, pl.ds(w, 1)] = quantize(v)
                    for copy in copies2(p, rb, bat):
                        copy.start()
                else:
                    for w, v in enumerate(values):
                        mid[p][bat * WIDTH + w] = v

    def copies3(p, k):
        device = peer(p, 2, k)
        return (
            remote(q3[p].at[k - 1], r3[p].at[k - 1], sem3.at[p, k - 1, 0], device),
            remote(t3[p].at[k - 1], u3[p].at[k - 1], sem3.at[p, k - 1, 1], device),
        )

    def third_dim(bat):
        for p in range(3):
            for k in (1, 3, 2):
                for copy in copies2(p, k, bat):
                    copy.wait_recv()
            values = []
            for w in range(WIDTH):
                c = bat * WIDTH + w
                v = mid[p][c]
                for k in range(3):
                    v = v + restored(r2[p][k, c], u2[p][k, bat, pl.ds(w, 1)])
                values.append(v)
            for w, v in enumerate(values):
                rc = ORDER[bat * WIDTH + w]
                if rc:
                    q3[p][rc - 1], t3[p][rc - 1, pl.ds(0, 1)] = quantize(v)
                    for copy in copies3(p, rc):
                        copy.start()
                else:
                    mid[p][3] = v

    def count_sources():
        for copy in count_far:
            copy.wait_recv()
        loads = table[...].reshape(128, 128).T[:64]
        expert = lax.broadcasted_iota(jnp.int32, (64, 128), 0)
        first = (e * 8 + r) * 8
        found = []
        for g in range(8):
            group = owner[first + g]
            place = lax.broadcasted_iota(jnp.int32, (GROUP, 128), 0) + lax.rem(group, 16) * GROUP
            load_line = jnp.sum(jnp.where(expert == lax.div(group, 16), loads, 0.0), axis=0, keepdims=True)
            live = jnp.where(load_line > place.astype(jnp.float32), 1.0, 0.0)
            found.append(jnp.maximum(jnp.sum(live, axis=1, keepdims=True), 1.0))
        for g in range(8):
            times[pl.ds(g * GROUP, GROUP)] = jnp.broadcast_to(found[g], (GROUP, 128))

    for k in (0, 1, 2):
        gather(0, k)
    fs_copy.wait_recv()
    expand(far_lived, far_lines)
    first_dim(0, FAR)
    for k in (0, 1, 2):
        gather(1, k)
    first_dim(0, OWN)
    mine = tile[...]
    for j, copy in enumerate(count_near):
        copy.wait_recv()
        mine = mine + tiles[j]
    table[e] = mine
    for copy in count_far:
        copy.start()
    first_dim(1, FAR)
    gather(0, 3)
    first_dim(0, BOTH)
    gather(1, 3)
    first_dim(1, OWN)
    own_share(0)
    first_dim(1, BOTH)
    own_share(1)
    second_dim(0)
    second_dim(1)
    count_sources()
    third_dim(0)
    third_dim(1)

    square = jnp.zeros((8, 128), jnp.float32)
    for p in range(3):
        n = ROWS[p]
        for k in (1, 3, 2):
            for copy in copies3(p, k):
                copy.wait_recv()
        v = mid[p][3]
        for k in range(3):
            v = v + restored(r3[p][k], u3[p][k, pl.ds(0, 1)])
        mean = v / times[pl.ds(START[p], n)]
        avg[pl.ds(START[p], n)] = mean
        square = square + jnp.sum((mean * mean).reshape(n // 8, 8, 128), axis=0)

    total = jnp.sum(square, axis=0, keepdims=True)
    red_send[0] = total
    red_copies = [remote(red_send.at[0], red_near.at[j], near_sem.at[1, j], near_peers[j]) for j in range(7)]
    for copy in red_copies:
        copy.start()
    for j, copy in enumerate(red_copies):
        copy.wait_recv()
        total = total + red_near[j]
    red_send[1] = total
    red_copies2 = [remote(red_send.at[1], red_far.at[j], far_sem.at[1, j], far_peers[j]) for j in range(15)]
    for copy in red_copies2:
        copy.start()
    for j, copy in enumerate(red_copies2):
        copy.wait_recv()
        total = total + red_far[j]
    root_mean = jnp.sqrt(jnp.sum(total, axis=1, keepdims=True) / (32768 * 128) + EPS)
    factor = jnp.minimum(1.0, CLIP / root_mean)
    for h in range(2):
        clipped = avg[pl.ds(h * 128, 128)] * factor
        top = jnp.max(jnp.abs(clipped), axis=1, keepdims=True) + EPS
        out[pl.ds(h * 128, 128)] = (clipped / top).astype(jnp.bfloat16)
        peak[pl.ds(h, 1)] = jnp.sum(top * eye[...], axis=0, keepdims=True)

    fs_copy.wait_send()
    for copy in count_near + count_far + red_copies + red_copies2:
        copy.wait_send()
    for p in range(3):
        for bat in range(BATCHES):
            for k in range(4):
                pair_copy(p, k, bat).wait_send()
            for d in range(2):
                for kind in range(3):
                    for copy in copies1(p, d, kind, bat):
                        copy.wait_send()
            for k in (1, 2, 3):
                for copy in copies2(p, k, bat):
                    copy.wait_send()
        for k in (1, 2, 3):
            for copy in copies3(p, k):
                copy.wait_send()


def scratch():
    f32, bf16, i16 = jnp.float32, jnp.bfloat16, jnp.int16

    def each(shape, dtype):
        return [pltpu.VMEM(shape(n), dtype) for n in ROWS]

    shapes = [
        pltpu.VMEM((1024, GROUP, 128), bf16),
        pltpu.VMEM((128, 128), f32),
        pltpu.VMEM((256, 128), f32),
        pltpu.VMEM((256, 128), f32),
        pltpu.VMEM((4, 256, 128), f32),
        pltpu.VMEM((1024, 1, 128), f32),
        pltpu.VMEM((1024, 1, 128), f32),
        pltpu.VMEM((8, 128), f32),
        pltpu.VMEM((7, 8, 128), f32),
        pltpu.VMEM((16, 8, 128), f32),
        pltpu.VMEM((256, 128), f32),
        pltpu.VMEM((2, 1, 128), f32),
        pltpu.VMEM((7, 1, 128), f32),
        pltpu.VMEM((15, 1, 128), f32),
        pltpu.VMEM((256, 128), f32),
    ]
    shapes += each(lambda n: (4, 16, n, 128), bf16) * 2
    shapes += each(lambda n: (16, n, 128), f32)
    shapes += each(lambda n: (2, 3, 8, n, 128), i16) * 2
    shapes += each(lambda n: (2, 3, BATCHES, 8, 128), f32) * 2
    shapes += each(lambda n: (4, n, 128), f32)
    shapes += each(lambda n: (3, 4, n, 128), i16) * 2
    shapes += each(lambda n: (3, BATCHES, 8, 128), f32) * 2
    shapes += each(lambda n: (3, n, 128), i16) * 2
    shapes += each(lambda n: (3, 8, 128), f32) * 2
    dma = pltpu.SemaphoreType.DMA
    shapes += [dma((LOADS,)), dma((3, 4, BATCHES, 2)), dma((2,)), dma((3, 2, 3, BATCHES, 2, 2)),
               dma((3, 3, BATCHES, 2, 2)), dma((3, 3, 2, 2)), dma((2, 7, 2)), dma((2, 15, 2))]
    return shapes


def local(mantissa, scales, counts, owner_map):
    vmem, smem = pl.BlockSpec(memory_space=pltpu.VMEM), pl.BlockSpec(memory_space=pltpu.SMEM)
    out, peak = pl.pallas_call(
        kernel,
        out_shape=(jax.ShapeDtypeStruct((256, 128), jnp.bfloat16), jax.ShapeDtypeStruct((2, 128), jnp.float32)),
        in_specs=[smem, smem, pl.BlockSpec(memory_space=pl.ANY), vmem, vmem],
        out_specs=(vmem, vmem),
        scratch_shapes=scratch(),
        compiler_params=pltpu.CompilerParams(
            collective_id=0, has_side_effects=True, vmem_limit_bytes=60 * 1024 * 1024
        ),
    )(owner_map, counts, mantissa.reshape(1024, GROUP, 128), scales.reshape(256, 128), counts.reshape(1, 64))
    return out, peak.reshape(256)


def solution(mesh):
    return jax.shard_map(
        local,
        mesh=mesh,
        in_specs=(P(AXES, None), P(AXES), P(AXES), P()),
        out_specs=(P(AXES, None), P(AXES)),
        check_vma=False,
    )
```

```python
import jax
import jax.numpy as jnp
from jax import lax
from jax.experimental import pallas as pl
from jax.experimental.pallas import tpu as pltpu
from jax.sharding import PartitionSpec as P

MESH = pl.DeviceIdType.MESH
AXES = ("expert", "replica")
GROUP = 32
CLIP = 0.05
EPS = 1e-06
ROWS = (96, 80, 80)
START = (0, 96, 176)
PIECES = (
    ((0, 0, 32), (1, 0, 32), (2, 0, 32)),
    ((3, 0, 32), (4, 0, 32), (5, 0, 16)),
    ((5, 16, 16), (6, 0, 32), (7, 0, 32)),
)
ORDER = (2, 1, 3, 0)
BATCHES = 2
WIDTH = 4 // BATCHES
FAR, OWN, BOTH = 0, 1, 2
TOP = 32767.0
LOADS = 8


def pick(k, a, b, c):
    return a * ((1 - k) * (2 - k) // 2) + b * (k * (2 - k)) + c * (k * (k - 1) // 2)


def kernel(owner, counts, mant_hbm, scales, count_row, avg, total_out, *rest):
    rest = list(rest)

    def take(n):
        head = rest[:n]
        del rest[:n]
        return head

    mant, eye, lived, far_lived, turned, lines, far_lines = take(7)
    tile, tiles, table, times, red_send, red_near, red_far = take(7)
    dsend, drecv, own = take(3), take(3), take(3)
    q1, r1, t1, u1 = take(3), take(3), take(3), take(3)
    mid = take(3)
    q2, r2, t2, u2 = take(3), take(3), take(3), take(3)
    q3, r3, t3, u3 = take(3), take(3), take(3), take(3)
    load_sem, pair_sem, fs_sem, sem1, sem2, sem3, near_sem, far_sem = rest

    e, r = lax.axis_index("expert"), lax.axis_index("replica")
    z, x = lax.div(e, 4), lax.rem(e, 4)
    y, core = lax.div(r, 2), lax.rem(r, 2)
    partner = (e, y * 2 + 1 - core)

    turns = [[lax.rem(v + rel, 4) for rel in range(4)] for v in (x, y, z)]
    weights = (64, 16, 256)

    def turned_by(c):
        return [
            [pick(lax.rem(dim + c, 3), *(turns[i][rel] * weights[i] for i in range(3))) for rel in range(4)]
            for dim in range(3)
        ]

    mine_at, other_at = turned_by(core), turned_by(1 - core)

    def first_group(c, p, ra, rb, rc):
        at = mine_at if c == 0 else other_at
        own_core = core if c == 0 else 1 - core
        return at[p][ra] + at[(p + 1) % 3][rb] + at[(p + 2) % 3][rc] + own_core * 8

    def peer(p, role, rel):
        dim = lax.rem((p + role) % 3 + core, 3)
        x2, y2, z2 = (
            pick(lax.rem(dim + 3 - i, 3), turns[i][rel], turns[i][0], turns[i][0]) for i in range(3)
        )
        return (z2 * 4 + x2, y2 * 2 + core)

    def remote(src, dst, sems, device):
        return pltpu.make_async_remote_copy(
            src_ref=src, dst_ref=dst, send_sem=sems.at[0], recv_sem=sems.at[1],
            device_id=device, device_id_type=MESH,
        )

    def load(i):
        part = pl.ds(i * (1024 // LOADS), 1024 // LOADS)
        return pltpu.make_async_copy(mant_hbm.at[part], mant.at[part], load_sem.at[i])

    for i in range(LOADS):
        load(i).start()

    near_peers = [(e, lax.rem(r + j, 8)) for j in range(1, 8)]
    far_peers = [(lax.rem(e + j, 16), r) for j in range(1, 16)]
    barrier = pltpu.get_barrier_semaphore()
    for device in near_peers + far_peers:
        pl.semaphore_signal(barrier, inc=1, device_id=device, device_id_type=MESH)

    row16 = lax.broadcasted_iota(jnp.int32, (16, 128), 0)
    lane16 = lax.broadcasted_iota(jnp.int32, (16, 128), 1)
    spot = lane16 + lax.rem(row16, 4) * 128
    which = lax.div(row16, 4)

    @pl.loop(0, 16)
    def _(b):
        bound = jnp.where(which < 2, jnp.where(which == 0, counts[b * 4], counts[b * 4 + 1]),
                          jnp.where(which == 2, counts[b * 4 + 2], counts[b * 4 + 3]))
        rows = pl.ds(pl.multiple_of(b * 16, 16), 16)
        lived[rows] = jnp.where(spot < bound, scales[rows].astype(jnp.float32), 0.0)

    def expand(source, target):
        for q in range(4):
            lanes = source[...] if q == 0 else pltpu.roll(source[...], 128 - q * GROUP, 1)
            turned[q] = jnp.where(lax.broadcasted_iota(jnp.int32, (256, 128), 1) < GROUP, lanes, 0.0)

        @pl.loop(0, 32)
        def _(b):
            for i in range(8):
                for q in range(4):
                    target[(b * 8 + i) * 4 + q] = turned[q, pl.ds(b * 8 + i, 1)]

    eye[...] = jnp.where(
        lax.broadcasted_iota(jnp.int32, (128, 128), 0) == lax.broadcasted_iota(jnp.int32, (128, 128), 1), 1.0, 0.0
    )
    row8 = lax.broadcasted_iota(jnp.int32, (8, 128), 0)
    tile[...] = jnp.zeros((8, 128), jnp.float32)
    tile[:, pl.ds(0, 64)] = jnp.where(row8[:, :64] == r, jnp.broadcast_to(count_row[...].astype(jnp.float32), (8, 64)), 0.0)
    pl.semaphore_wait(barrier, 22)

    fs_copy = remote(lived, far_lived, fs_sem, partner)
    fs_copy.start()
    count_near = [remote(tile, tiles.at[j], near_sem.at[0, j], near_peers[j]) for j in range(7)]
    count_far = [remote(table.at[e], table.at[e], far_sem.at[0, j], far_peers[j]) for j in range(15)]
    for copy in count_near:
        copy.start()
    expand(lived, lines)
    for i in range(LOADS):
        load(i).wait()

    def pair_copy(p, k, bat):
        part = pl.ds(bat * WIDTH * 4, WIDTH * 4)
        return remote(dsend[p].at[k, part], drecv[p].at[k, part], pair_sem.at[p, k, bat], partner)

    def gather(bat, k):
        for p in range(3):
            for c in range(bat * WIDTH, (bat + 1) * WIDTH):
                for rb in range(4):
                    first = first_group(1, p, ORDER[k], rb, ORDER[c])
                    at = 0
                    for g, r0, n in PIECES[p]:
                        dsend[p][k, c * 4 + rb, pl.ds(at, n)] = mant[owner[first + g], pl.ds(r0, n)]
                        at += n
            pair_copy(p, k, bat).start()

    lane = lax.broadcasted_iota(jnp.int32, (1, 128), 1)

    def scale_row(source, groups, p):
        row, at = None, 0
        for group, (_, r0, n) in zip(groups, PIECES[p]):
            piece = source[group]
            if n < GROUP:
                piece = jnp.where(lane < n, piece, 0.0) if r0 == 0 else jnp.where(lane < r0, 0.0, piece)
            if at != r0:
                piece = pltpu.roll(piece, (at - r0) % 128, 1)
            row = piece if row is None else row + piece
            at += n
        return row

    def scaled(row, rows):
        n = rows.shape[0]
        weight = (eye[pl.ds(0, n)] * row).astype(jnp.bfloat16)[:, :n]
        return jnp.dot(weight, rows, preferred_element_type=jnp.float32)

    def product(p, k, rb, c):
        first = first_group(0, p, ORDER[k], rb, ORDER[c])
        groups = [owner[first + g] for g, _, _ in PIECES[p]]
        mine = jnp.concatenate([mant[group, pl.ds(r0, n)] for group, (_, r0, n) in zip(groups, PIECES[p])], axis=0)
        other = drecv[p][k, c * 4 + rb]
        return scaled(scale_row(lines, groups, p), mine) + scaled(scale_row(far_lines, groups, p), other)

    def quantize(v):
        n = v.shape[0]
        most = jnp.maximum(jnp.max(jnp.abs(v), axis=1, keepdims=True), 1e-30)
        step = (most * (1.0045 / TOP)).astype(jnp.bfloat16).astype(jnp.float32)
        q = lax.round(v / step, lax.RoundingMethod.TO_NEAREST_EVEN)
        row = jnp.sum(step * eye[pl.ds(0, n)], axis=0, keepdims=True)
        return q.astype(jnp.int32).astype(jnp.int16), row

    def restored(q, row):
        n = q.shape[0]
        weight = (eye[pl.ds(0, n)] * row).astype(jnp.bfloat16)
        step = jnp.dot(weight, jnp.ones((128, 128), jnp.bfloat16), preferred_element_type=jnp.float32)
        return q.astype(jnp.int32).astype(jnp.float32) * step

    def copies1(p, d, kind, bat):
        device = peer(p, 0, 1 + 2 * d)
        part = pl.ds(bat * WIDTH * 2, WIDTH * 2)
        return (
            remote(q1[p].at[d, kind, part], r1[p].at[d, kind, part], sem1.at[p, d, kind, bat, 0], device),
            remote(t1[p].at[d, kind, bat], u1[p].at[d, kind, bat], sem1.at[p, d, kind, bat, 1], device),
        )

    def places(bat):
        return [(c, i) for c in range(bat * WIDTH, (bat + 1) * WIDTH) for i in range(2)]

    def first_dim(bat, kind):
        for p in range(3):
            if kind == FAR:
                pair_copy(p, 0, bat).wait_recv()
            if kind == OWN:
                pair_copy(p, 1, bat).wait_recv()
                pair_copy(p, 2, bat).wait_recv()
            if kind == BOTH:
                for d in range(2):
                    for copy in copies1(p, d, FAR, bat):
                        copy.wait_recv()
            coded = []
            for d in range(2):
                half = 1 - d if kind == OWN else d
                for j, (c, i) in enumerate(places(bat)):
                    v = product(p, 0 if kind == FAR else 1 + d, half * 2 + i, c)
                    if kind == BOTH:
                        v = v + restored(r1[p][d, FAR, c * 2 + i], u1[p][d, FAR, bat, pl.ds(j, 1)])
                    coded.append((d, c * 2 + i, j, quantize(v)))
            for d, u, j, (q, step) in coded:
                q1[p][d, kind, u] = q
                t1[p][d, kind, bat, pl.ds(j, 1)] = step
            for d in range(2):
                for copy in copies1(p, d, kind, bat):
                    copy.start()

    def own_share(bat):
        for p in range(3):
            pair_copy(p, 3, bat).wait_recv()
            for c in range(bat * WIDTH, (bat + 1) * WIDTH):
                values = [product(p, 3, rb, c) for rb in range(4)]
                for rb in range(4):
                    own[p][c * 4 + rb] = values[rb]

    def copies2(p, k, bat):
        device = peer(p, 1, k)
        part = pl.ds(bat * WIDTH, WIDTH)
        return (
            remote(q2[p].at[k - 1, part], r2[p].at[k - 1, part], sem2.at[p, k - 1, bat, 0], device),
            remote(t2[p].at[k - 1, bat], u2[p].at[k - 1, bat], sem2.at[p, k - 1, bat, 1], device),
        )

    def second_dim(bat):
        for p in range(3):
            for d in range(2):
                for kind in (OWN, BOTH):
                    for copy in copies1(p, d, kind, bat):
                        copy.wait_recv()
            for rb in ORDER:
                h, values = rb // 2, []
                for w in range(WIDTH):
                    c = bat * WIDTH + w
                    v = own[p][c * 4 + rb]
                    for d, kind in ((h, BOTH), (1 - h, OWN)):
                        v = v + restored(r1[p][d, kind, c * 2 + rb % 2], u1[p][d, kind, bat, pl.ds(w * 2 + rb % 2, 1)])
                    values.append(v)
                if rb:
                    for w, v in enumerate(values):
                        q2[p][rb - 1, bat * WIDTH + w], t2[p][rb - 1, bat, pl.ds(w, 1)] = quantize(v)
                    for copy in copies2(p, rb, bat):
                        copy.start()
                else:
                    for w, v in enumerate(values):
                        mid[p][bat * WIDTH + w] = v

    def copies3(p, k):
        device = peer(p, 2, k)
        return (
            remote(q3[p].at[k - 1], r3[p].at[k - 1], sem3.at[p, k - 1, 0], device),
            remote(t3[p].at[k - 1], u3[p].at[k - 1], sem3.at[p, k - 1, 1], device),
        )

    def third_dim(bat):
        for p in range(3):
            for k in (1, 3, 2):
                for copy in copies2(p, k, bat):
                    copy.wait_recv()
            values = []
            for w in range(WIDTH):
                c = bat * WIDTH + w
                v = mid[p][c]
                for k in range(3):
                    v = v + restored(r2[p][k, c], u2[p][k, bat, pl.ds(w, 1)])
                values.append(v)
            for w, v in enumerate(values):
                rc = ORDER[bat * WIDTH + w]
                if rc:
                    q3[p][rc - 1], t3[p][rc - 1] = quantize(v)
                    for copy in copies3(p, rc):
                        copy.start()
                else:
                    mid[p][3] = v

    def count_sources():
        for copy in count_far:
            copy.wait_recv()
        loads = table[...].reshape(128, 128).T[:64]
        expert = lax.broadcasted_iota(jnp.int32, (64, 128), 0)
        first = (e * 8 + r) * 8
        found = []
        for g in range(8):
            group = owner[first + g]
            place = lax.broadcasted_iota(jnp.int32, (GROUP, 128), 0) + lax.rem(group, 16) * GROUP
            load_line = jnp.sum(jnp.where(expert == lax.div(group, 16), loads, 0.0), axis=0, keepdims=True)
            live = jnp.where(load_line > place.astype(jnp.float32), 1.0, 0.0)
            found.append(jnp.maximum(jnp.sum(live, axis=1, keepdims=True), 1.0))
        for g in range(8):
            times[pl.ds(g * GROUP, GROUP)] = jnp.broadcast_to(found[g], (GROUP, 128))

    for k in (0, 1, 2):
        gather(0, k)
    fs_copy.wait_recv()
    expand(far_lived, far_lines)
    first_dim(0, FAR)
    for k in (0, 1, 2):
        gather(1, k)
    first_dim(0, OWN)
    mine = tile[...]
    for j, copy in enumerate(count_near):
        copy.wait_recv()
        mine = mine + tiles[j]
    table[e] = mine
    for copy in count_far:
        copy.start()
    first_dim(1, FAR)
    gather(0, 3)
    first_dim(0, BOTH)
    gather(1, 3)
    first_dim(1, OWN)
    own_share(0)
    first_dim(1, BOTH)
    own_share(1)
    second_dim(0)
    second_dim(1)
    count_sources()
    third_dim(0)
    third_dim(1)

    square = jnp.zeros((8, 128), jnp.float32)
    for p in range(3):
        n = ROWS[p]
        for k in (1, 3, 2):
            for copy in copies3(p, k):
                copy.wait_recv()
        v = mid[p][3]
        for k in range(3):
            v = v + restored(r3[p][k], u3[p][k])
        mean = v / times[pl.ds(START[p], n)]
        avg[pl.ds(START[p], n)] = mean
        square = square + jnp.sum((mean * mean).reshape(n // 8, 8, 128), axis=0)

    total = jnp.sum(square, axis=0, keepdims=True)
    red_send[0] = total
    red_copies = [remote(red_send.at[0], red_near.at[j], near_sem.at[1, j], near_peers[j]) for j in range(7)]
    for copy in red_copies:
        copy.start()
    for j, copy in enumerate(red_copies):
        copy.wait_recv()
        total = total + red_near[j]
    red_send[1] = total
    red_copies2 = [remote(red_send.at[1], red_far.at[j], far_sem.at[1, j], far_peers[j]) for j in range(15)]
    for copy in red_copies2:
        copy.start()
    for j, copy in enumerate(red_copies2):
        copy.wait_recv()
        total = total + red_far[j]
    total_out[...] = total

    fs_copy.wait_send()
    for copy in count_near + count_far + red_copies + red_copies2:
        copy.wait_send()
    for p in range(3):
        for bat in range(BATCHES):
            for k in range(4):
                pair_copy(p, k, bat).wait_send()
            for d in range(2):
                for kind in range(3):
                    for copy in copies1(p, d, kind, bat):
                        copy.wait_send()
            for k in (1, 2, 3):
                for copy in copies2(p, k, bat):
                    copy.wait_send()
        for k in (1, 2, 3):
            for copy in copies3(p, k):
                copy.wait_send()


def finish(avg, total, out, peak):
    root_mean = jnp.sqrt(jnp.sum(total[...], axis=1, keepdims=True) / (32768 * 128) + EPS)
    factor = jnp.minimum(1.0, CLIP / root_mean)
    same = lax.broadcasted_iota(jnp.int32, (128, 128), 0) == lax.broadcasted_iota(jnp.int32, (128, 128), 1)
    for h in range(2):
        clipped = avg[pl.ds(h * 128, 128)] * factor
        top = jnp.max(jnp.abs(clipped), axis=1, keepdims=True) + EPS
        out[pl.ds(h * 128, 128)] = (clipped / top).astype(jnp.bfloat16)
        peak[pl.ds(h, 1)] = jnp.sum(jnp.where(same, top, 0.0), axis=0, keepdims=True)


def scratch():
    f32, bf16, i16 = jnp.float32, jnp.bfloat16, jnp.int16

    def each(shape, dtype):
        return [pltpu.VMEM(shape(n), dtype) for n in ROWS]

    shapes = [
        pltpu.VMEM((1024, GROUP, 128), bf16),
        pltpu.VMEM((128, 128), f32),
        pltpu.VMEM((256, 128), f32),
        pltpu.VMEM((256, 128), f32),
        pltpu.VMEM((4, 256, 128), f32),
        pltpu.VMEM((1024, 1, 128), f32),
        pltpu.VMEM((1024, 1, 128), f32),
        pltpu.VMEM((8, 128), f32),
        pltpu.VMEM((7, 8, 128), f32),
        pltpu.VMEM((16, 8, 128), f32),
        pltpu.VMEM((256, 128), f32),
        pltpu.VMEM((2, 1, 128), f32),
        pltpu.VMEM((7, 1, 128), f32),
        pltpu.VMEM((15, 1, 128), f32),
    ]
    shapes += each(lambda n: (4, 16, n, 128), bf16) * 2
    shapes += each(lambda n: (16, n, 128), f32)
    shapes += each(lambda n: (2, 3, 8, n, 128), i16) * 2
    shapes += each(lambda n: (2, 3, BATCHES, WIDTH * 2, 128), f32) * 2
    shapes += each(lambda n: (4, n, 128), f32)
    shapes += each(lambda n: (3, 4, n, 128), i16) * 2
    shapes += each(lambda n: (3, BATCHES, WIDTH, 128), f32) * 2
    shapes += each(lambda n: (3, n, 128), i16) * 2
    shapes += each(lambda n: (3, 1, 128), f32) * 2
    dma = pltpu.SemaphoreType.DMA
    shapes += [dma((LOADS,)), dma((3, 4, BATCHES, 2)), dma((2,)), dma((3, 2, 3, BATCHES, 2, 2)),
               dma((3, 3, BATCHES, 2, 2)), dma((3, 3, 2, 2)), dma((2, 7, 2)), dma((2, 15, 2))]
    return shapes


def local(mantissa, scales, counts, owner_map):
    vmem, smem = pl.BlockSpec(memory_space=pltpu.VMEM), pl.BlockSpec(memory_space=pltpu.SMEM)
    averaged, total = pl.pallas_call(
        kernel,
        out_shape=(jax.ShapeDtypeStruct((256, 128), jnp.float32), jax.ShapeDtypeStruct((1, 128), jnp.float32)),
        in_specs=[smem, smem, pl.BlockSpec(memory_space=pl.ANY), vmem, vmem],
        out_specs=(vmem, vmem),
        scratch_shapes=scratch(),
        compiler_params=pltpu.CompilerParams(
            collective_id=0, has_side_effects=True, vmem_limit_bytes=60 * 1024 * 1024
        ),
    )(owner_map, counts, mantissa.reshape(1024, GROUP, 128), scales.reshape(256, 128), counts.reshape(1, 64))
    out, peak = pl.pallas_call(
        finish,
        out_shape=(jax.ShapeDtypeStruct((256, 128), jnp.bfloat16), jax.ShapeDtypeStruct((2, 128), jnp.float32)),
        in_specs=[vmem, vmem],
        out_specs=(vmem, vmem),
    )(averaged, total)
    return out, peak.reshape(256)


def solution(mesh):
    return jax.shard_map(
        local,
        mesh=mesh,
        in_specs=(P(AXES, None), P(AXES), P(AXES), P()),
        out_specs=(P(AXES, None), P(AXES)),
        check_vma=False,
    )
```

```python
import jax
import jax.numpy as jnp
from jax import lax
from jax.experimental import pallas as pl
from jax.experimental.pallas import tpu as pltpu
from jax.sharding import PartitionSpec as P

MESH = pl.DeviceIdType.MESH
AXES = ("expert", "replica")
GROUP = 32
CLIP = 0.05
EPS = 1e-06
ROWS = (96, 80, 80)
START = (0, 96, 176)
PIECES = (
    ((0, 0, 32), (1, 0, 32), (2, 0, 32)),
    ((3, 0, 32), (4, 0, 32), (5, 0, 16)),
    ((5, 16, 16), (6, 0, 32), (7, 0, 32)),
)
ORDER = (2, 1, 3, 0)
BATCHES = 2
WIDTH = 4 // BATCHES
FAR, OWN, BOTH = 0, 1, 2
TOP = 32767.0
LOADS = 8


def pick(k, a, b, c):
    return a * ((1 - k) * (2 - k) // 2) + b * (k * (2 - k)) + c * (k * (k - 1) // 2)


def kernel(owner, counts, mant_hbm, scales, count_row, avg, total_out, *rest):
    rest = list(rest)

    def take(n):
        head = rest[:n]
        del rest[:n]
        return head

    mant, eye, lived, far_lived, turned, lines, far_lines = take(7)
    tile, tiles, table, times, red_send, red_near, red_far = take(7)
    dsend, drecv, own = take(3), take(3), take(3)
    q1, r1, t1, u1 = take(3), take(3), take(3), take(3)
    mid = take(3)
    q2, r2, t2, u2 = take(3), take(3), take(3), take(3)
    q3, r3, t3, u3 = take(3), take(3), take(3), take(3)
    load_sem, pair_sem, fs_sem, sem1, sem2, sem3, near_sem, far_sem = rest

    e, r = lax.axis_index("expert"), lax.axis_index("replica")
    z, x = lax.div(e, 4), lax.rem(e, 4)
    y, core = lax.div(r, 2), lax.rem(r, 2)
    partner = (e, y * 2 + 1 - core)

    turns = [[lax.rem(v + rel, 4) for rel in range(4)] for v in (x, y, z)]
    weights = (64, 16, 256)

    def turned_by(c):
        return [
            [pick(lax.rem(dim + c, 3), *(turns[i][rel] * weights[i] for i in range(3))) for rel in range(4)]
            for dim in range(3)
        ]

    mine_at, other_at = turned_by(core), turned_by(1 - core)

    def first_group(c, p, ra, rb, rc):
        at = mine_at if c == 0 else other_at
        own_core = core if c == 0 else 1 - core
        return at[p][ra] + at[(p + 1) % 3][rb] + at[(p + 2) % 3][rc] + own_core * 8

    def peer(p, role, rel):
        dim = lax.rem((p + role) % 3 + core, 3)
        x2, y2, z2 = (
            pick(lax.rem(dim + 3 - i, 3), turns[i][rel], turns[i][0], turns[i][0]) for i in range(3)
        )
        return (z2 * 4 + x2, y2 * 2 + core)

    def remote(src, dst, sems, device):
        return pltpu.make_async_remote_copy(
            src_ref=src, dst_ref=dst, send_sem=sems.at[0], recv_sem=sems.at[1],
            device_id=device, device_id_type=MESH,
        )

    def load(i):
        part = pl.ds(i * (1024 // LOADS), 1024 // LOADS)
        return pltpu.make_async_copy(mant_hbm.at[part], mant.at[part], load_sem.at[i])

    for i in range(LOADS):
        load(i).start()

    near_peers = [(e, lax.rem(r + j, 8)) for j in range(1, 8)]
    far_peers = [(lax.rem(e + j, 16), r) for j in range(1, 16)]
    barrier = pltpu.get_barrier_semaphore()
    for device in near_peers + far_peers:
        pl.semaphore_signal(barrier, inc=1, device_id=device, device_id_type=MESH)

    row16 = lax.broadcasted_iota(jnp.int32, (16, 128), 0)
    lane16 = lax.broadcasted_iota(jnp.int32, (16, 128), 1)
    spot = lane16 + lax.rem(row16, 4) * 128
    which = lax.div(row16, 4)

    @pl.loop(0, 16)
    def _(b):
        bound = jnp.where(which < 2, jnp.where(which == 0, counts[b * 4], counts[b * 4 + 1]),
                          jnp.where(which == 2, counts[b * 4 + 2], counts[b * 4 + 3]))
        rows = pl.ds(pl.multiple_of(b * 16, 16), 16)
        lived[rows] = jnp.where(spot < bound, scales[rows].astype(jnp.float32), 0.0)

    def expand(source, target):
        for q in range(4):
            lanes = source[...] if q == 0 else pltpu.roll(source[...], 128 - q * GROUP, 1)
            turned[q] = jnp.where(lax.broadcasted_iota(jnp.int32, (256, 128), 1) < GROUP, lanes, 0.0)

        @pl.loop(0, 32)
        def _(b):
            for i in range(8):
                for q in range(4):
                    target[(b * 8 + i) * 4 + q] = turned[q, pl.ds(b * 8 + i, 1)]

    eye[...] = jnp.where(
        lax.broadcasted_iota(jnp.int32, (128, 128), 0) == lax.broadcasted_iota(jnp.int32, (128, 128), 1), 1.0, 0.0
    )
    row8 = lax.broadcasted_iota(jnp.int32, (8, 128), 0)
    tile[...] = jnp.zeros((8, 128), jnp.float32)
    tile[:, pl.ds(0, 64)] = jnp.where(row8[:, :64] == r, jnp.broadcast_to(count_row[...].astype(jnp.float32), (8, 64)), 0.0)
    pl.semaphore_wait(barrier, 22)

    fs_copy = remote(lived, far_lived, fs_sem, partner)
    fs_copy.start()
    count_near = [remote(tile, tiles.at[j], near_sem.at[0, j], near_peers[j]) for j in range(7)]
    count_far = [remote(table.at[e], table.at[e], far_sem.at[0, j], far_peers[j]) for j in range(15)]
    for copy in count_near:
        copy.start()
    expand(lived, lines)
    for i in range(LOADS):
        load(i).wait()

    def pair_copy(p, k, bat):
        part = pl.ds(bat * WIDTH * 4, WIDTH * 4)
        return remote(dsend[p].at[k, part], drecv[p].at[k, part], pair_sem.at[p, k, bat], partner)

    def gather(bat, k):
        for p in range(3):
            for c in range(bat * WIDTH, (bat + 1) * WIDTH):
                for rb in range(4):
                    first = first_group(1, p, ORDER[k], rb, ORDER[c])
                    at = 0
                    for g, r0, n in PIECES[p]:
                        dsend[p][k, c * 4 + rb, pl.ds(at, n)] = mant[owner[first + g], pl.ds(r0, n)]
                        at += n
            pair_copy(p, k, bat).start()

    lane = lax.broadcasted_iota(jnp.int32, (1, 128), 1)

    def scale_row(source, groups, p):
        row, at = None, 0
        for group, (_, r0, n) in zip(groups, PIECES[p]):
            piece = source[group]
            if n < GROUP:
                piece = jnp.where(lane < n, piece, 0.0) if r0 == 0 else jnp.where(lane < r0, 0.0, piece)
            if at != r0:
                piece = pltpu.roll(piece, (at - r0) % 128, 1)
            row = piece if row is None else row + piece
            at += n
        return row

    def scaled(row, rows):
        n = rows.shape[0]
        weight = (eye[pl.ds(0, n)] * row).astype(jnp.bfloat16)[:, :n]
        return jnp.dot(weight, rows, preferred_element_type=jnp.float32)

    def product(p, k, rb, c):
        first = first_group(0, p, ORDER[k], rb, ORDER[c])
        groups = [owner[first + g] for g, _, _ in PIECES[p]]
        mine = jnp.concatenate([mant[group, pl.ds(r0, n)] for group, (_, r0, n) in zip(groups, PIECES[p])], axis=0)
        other = drecv[p][k, c * 4 + rb]
        return scaled(scale_row(lines, groups, p), mine) + scaled(scale_row(far_lines, groups, p), other)

    def quantize(v):
        n = v.shape[0]
        most = jnp.maximum(jnp.max(jnp.abs(v), axis=1, keepdims=True), 1e-30)
        step = (most * (1.0045 / TOP)).astype(jnp.bfloat16).astype(jnp.float32)
        q = lax.round(v / step, lax.RoundingMethod.TO_NEAREST_EVEN)
        row = jnp.sum(step * eye[pl.ds(0, n)], axis=0, keepdims=True)
        return q.astype(jnp.int32).astype(jnp.int16), row

    def restored(q, row):
        n = q.shape[0]
        weight = (eye[pl.ds(0, n)] * row).astype(jnp.bfloat16)
        step = jnp.dot(weight, jnp.ones((128, 128), jnp.bfloat16), preferred_element_type=jnp.float32)
        return q.astype(jnp.int32).astype(jnp.float32) * step

    def copies1(p, d, kind, bat):
        device = peer(p, 0, 1 + 2 * d)
        part = pl.ds(bat * WIDTH * 2, WIDTH * 2)
        return (
            remote(q1[p].at[d, kind, part], r1[p].at[d, kind, part], sem1.at[p, d, kind, bat, 0], device),
            remote(t1[p].at[d, kind, bat], u1[p].at[d, kind, bat], sem1.at[p, d, kind, bat, 1], device),
        )

    def places(bat):
        return [(c, i) for c in range(bat * WIDTH, (bat + 1) * WIDTH) for i in range(2)]

    def first_dim(bat, kind):
        for p in range(3):
            if kind == FAR:
                pair_copy(p, 0, bat).wait_recv()
            if kind == OWN:
                pair_copy(p, 1, bat).wait_recv()
                pair_copy(p, 2, bat).wait_recv()
            if kind == BOTH:
                for d in range(2):
                    for copy in copies1(p, d, FAR, bat):
                        copy.wait_recv()
            coded = []
            for d in range(2):
                half = 1 - d if kind == OWN else d
                for j, (c, i) in enumerate(places(bat)):
                    v = product(p, 0 if kind == FAR else 1 + d, half * 2 + i, c)
                    if kind == BOTH:
                        v = v + restored(r1[p][d, FAR, c * 2 + i], u1[p][d, FAR, bat, pl.ds(j, 1)])
                    coded.append((d, c * 2 + i, j, quantize(v)))
            for d, u, j, (q, step) in coded:
                q1[p][d, kind, u] = q
                t1[p][d, kind, bat, pl.ds(j, 1)] = step
            for d in range(2):
                for copy in copies1(p, d, kind, bat):
                    copy.start()

    def own_share(bat):
        for p in range(3):
            pair_copy(p, 3, bat).wait_recv()
            for c in range(bat * WIDTH, (bat + 1) * WIDTH):
                values = [product(p, 3, rb, c) for rb in range(4)]
                for rb in range(4):
                    own[p][c * 4 + rb] = values[rb]

    def copies2(p, k, bat):
        device = peer(p, 1, k)
        part = pl.ds(bat * WIDTH, WIDTH)
        return (
            remote(q2[p].at[k - 1, part], r2[p].at[k - 1, part], sem2.at[p, k - 1, bat, 0], device),
            remote(t2[p].at[k - 1, bat], u2[p].at[k - 1, bat], sem2.at[p, k - 1, bat, 1], device),
        )

    def second_dim(bat):
        for p in range(3):
            for d in range(2):
                for kind in (OWN, BOTH):
                    for copy in copies1(p, d, kind, bat):
                        copy.wait_recv()
        coded, kept = [], []
        for p in range(3):
            for rb in ORDER:
                h = rb // 2
                for w in range(WIDTH):
                    c = bat * WIDTH + w
                    v = own[p][c * 4 + rb]
                    for d, kind in ((h, BOTH), (1 - h, OWN)):
                        v = v + restored(r1[p][d, kind, c * 2 + rb % 2], u1[p][d, kind, bat, pl.ds(w * 2 + rb % 2, 1)])
                    if rb:
                        coded.append((p, rb - 1, w, quantize(v)))
                    else:
                        kept.append((p, c, v))
        for p, k, w, (q, step) in coded:
            q2[p][k, bat * WIDTH + w] = q
            t2[p][k, bat, pl.ds(w, 1)] = step
        for p in range(3):
            for rb in (2, 1, 3):
                for copy in copies2(p, rb, bat):
                    copy.start()
        for p, c, v in kept:
            mid[p][c] = v

    def copies3(p, k):
        device = peer(p, 2, k)
        return (
            remote(q3[p].at[k - 1], r3[p].at[k - 1], sem3.at[p, k - 1, 0], device),
            remote(t3[p].at[k - 1], u3[p].at[k - 1], sem3.at[p, k - 1, 1], device),
        )

    def third_dim(bat):
        for p in range(3):
            for k in (1, 3, 2):
                for copy in copies2(p, k, bat):
                    copy.wait_recv()
        for w in range(WIDTH):
            c = bat * WIDTH + w
            sums = []
            for p in range(3):
                v = mid[p][c]
                for k in range(3):
                    v = v + restored(r2[p][k, c], u2[p][k, bat, pl.ds(w, 1)])
                sums.append(v)
            if ORDER[c]:
                coded = [quantize(v) for v in sums]
                for p, (q, step) in enumerate(coded):
                    q3[p][ORDER[c] - 1], t3[p][ORDER[c] - 1] = q, step
                for p in range(3):
                    for copy in copies3(p, ORDER[c]):
                        copy.start()
            else:
                for p in range(3):
                    mid[p][c] = sums[p]

    def count_sources():
        for copy in count_far:
            copy.wait_recv()
        loads = table[...].reshape(128, 128).T[:64]
        expert = lax.broadcasted_iota(jnp.int32, (64, 128), 0)
        first = (e * 8 + r) * 8
        found = []
        for g in range(8):
            group = owner[first + g]
            place = lax.broadcasted_iota(jnp.int32, (GROUP, 128), 0) + lax.rem(group, 16) * GROUP
            load_line = jnp.sum(jnp.where(expert == lax.div(group, 16), loads, 0.0), axis=0, keepdims=True)
            live = jnp.where(load_line > place.astype(jnp.float32), 1.0, 0.0)
            found.append(jnp.maximum(jnp.sum(live, axis=1, keepdims=True), 1.0))
        for g in range(8):
            times[pl.ds(g * GROUP, GROUP)] = jnp.broadcast_to(found[g], (GROUP, 128))

    for k in (0, 1, 2):
        gather(0, k)
    fs_copy.wait_recv()
    expand(far_lived, far_lines)
    first_dim(0, FAR)
    for k in (0, 1, 2):
        gather(1, k)
    first_dim(0, OWN)
    mine = tile[...]
    for j, copy in enumerate(count_near):
        copy.wait_recv()
        mine = mine + tiles[j]
    table[e] = mine
    for copy in count_far:
        copy.start()
    first_dim(1, FAR)
    gather(0, 3)
    first_dim(0, BOTH)
    gather(1, 3)
    first_dim(1, OWN)
    own_share(0)
    first_dim(1, BOTH)
    own_share(1)
    second_dim(0)
    second_dim(1)
    count_sources()
    third_dim(0)
    third_dim(1)

    for p in range(3):
        for k in (1, 3, 2):
            for copy in copies3(p, k):
                copy.wait_recv()
    square = jnp.zeros((8, 128), jnp.float32)
    means = []
    for p in range(3):
        v = mid[p][3]
        for k in range(3):
            v = v + restored(r3[p][k], u3[p][k])
        means.append(v / times[pl.ds(START[p], ROWS[p])])
    for mean in means:
        square = square + jnp.sum((mean * mean).reshape(mean.shape[0] // 8, 8, 128), axis=0)
    for p, mean in enumerate(means):
        avg[pl.ds(START[p], ROWS[p])] = mean

    total = jnp.sum(square, axis=0, keepdims=True)
    red_send[0] = total
    red_copies = [remote(red_send.at[0], red_near.at[j], near_sem.at[1, j], near_peers[j]) for j in range(7)]
    for copy in red_copies:
        copy.start()
    for j, copy in enumerate(red_copies):
        copy.wait_recv()
        total = total + red_near[j]
    red_send[1] = total
    red_copies2 = [remote(red_send.at[1], red_far.at[j], far_sem.at[1, j], far_peers[j]) for j in range(15)]
    for copy in red_copies2:
        copy.start()
    for j, copy in enumerate(red_copies2):
        copy.wait_recv()
        total = total + red_far[j]
    total_out[...] = total

    fs_copy.wait_send()
    for copy in count_near + count_far + red_copies + red_copies2:
        copy.wait_send()
    for p in range(3):
        for bat in range(BATCHES):
            for k in range(4):
                pair_copy(p, k, bat).wait_send()
            for d in range(2):
                for kind in range(3):
                    for copy in copies1(p, d, kind, bat):
                        copy.wait_send()
            for k in (1, 2, 3):
                for copy in copies2(p, k, bat):
                    copy.wait_send()
        for k in (1, 2, 3):
            for copy in copies3(p, k):
                copy.wait_send()


def finish(avg, total, out, peak):
    root_mean = jnp.sqrt(jnp.sum(total[...], axis=1, keepdims=True) / (32768 * 128) + EPS)
    factor = jnp.minimum(1.0, CLIP / root_mean)
    same = lax.broadcasted_iota(jnp.int32, (128, 128), 0) == lax.broadcasted_iota(jnp.int32, (128, 128), 1)
    for h in range(2):
        clipped = avg[pl.ds(h * 128, 128)] * factor
        top = jnp.max(jnp.abs(clipped), axis=1, keepdims=True) + EPS
        out[pl.ds(h * 128, 128)] = (clipped / top).astype(jnp.bfloat16)
        peak[pl.ds(h, 1)] = jnp.sum(jnp.where(same, top, 0.0), axis=0, keepdims=True)


def scratch():
    f32, bf16, i16 = jnp.float32, jnp.bfloat16, jnp.int16

    def each(shape, dtype):
        return [pltpu.VMEM(shape(n), dtype) for n in ROWS]

    shapes = [
        pltpu.VMEM((1024, GROUP, 128), bf16),
        pltpu.VMEM((128, 128), f32),
        pltpu.VMEM((256, 128), f32),
        pltpu.VMEM((256, 128), f32),
        pltpu.VMEM((4, 256, 128), f32),
        pltpu.VMEM((1024, 1, 128), f32),
        pltpu.VMEM((1024, 1, 128), f32),
        pltpu.VMEM((8, 128), f32),
        pltpu.VMEM((7, 8, 128), f32),
        pltpu.VMEM((16, 8, 128), f32),
        pltpu.VMEM((256, 128), f32),
        pltpu.VMEM((2, 1, 128), f32),
        pltpu.VMEM((7, 1, 128), f32),
        pltpu.VMEM((15, 1, 128), f32),
    ]
    shapes += each(lambda n: (4, 16, n, 128), bf16) * 2
    shapes += each(lambda n: (16, n, 128), f32)
    shapes += each(lambda n: (2, 3, 8, n, 128), i16) * 2
    shapes += each(lambda n: (2, 3, BATCHES, WIDTH * 2, 128), f32) * 2
    shapes += each(lambda n: (4, n, 128), f32)
    shapes += each(lambda n: (3, 4, n, 128), i16) * 2
    shapes += each(lambda n: (3, BATCHES, WIDTH, 128), f32) * 2
    shapes += each(lambda n: (3, n, 128), i16) * 2
    shapes += each(lambda n: (3, 1, 128), f32) * 2
    dma = pltpu.SemaphoreType.DMA
    shapes += [dma((LOADS,)), dma((3, 4, BATCHES, 2)), dma((2,)), dma((3, 2, 3, BATCHES, 2, 2)),
               dma((3, 3, BATCHES, 2, 2)), dma((3, 3, 2, 2)), dma((2, 7, 2)), dma((2, 15, 2))]
    return shapes


def local(mantissa, scales, counts, owner_map):
    vmem, smem = pl.BlockSpec(memory_space=pltpu.VMEM), pl.BlockSpec(memory_space=pltpu.SMEM)
    averaged, total = pl.pallas_call(
        kernel,
        out_shape=(jax.ShapeDtypeStruct((256, 128), jnp.float32), jax.ShapeDtypeStruct((1, 128), jnp.float32)),
        in_specs=[smem, smem, pl.BlockSpec(memory_space=pl.ANY), vmem, vmem],
        out_specs=(vmem, vmem),
        scratch_shapes=scratch(),
        compiler_params=pltpu.CompilerParams(
            collective_id=0, has_side_effects=True, vmem_limit_bytes=60 * 1024 * 1024
        ),
    )(owner_map, counts, mantissa.reshape(1024, GROUP, 128), scales.reshape(256, 128), counts.reshape(1, 64))
    out, peak = pl.pallas_call(
        finish,
        out_shape=(jax.ShapeDtypeStruct((256, 128), jnp.bfloat16), jax.ShapeDtypeStruct((2, 128), jnp.float32)),
        in_specs=[vmem, vmem],
        out_specs=(vmem, vmem),
    )(averaged, total)
    return out, peak.reshape(256)


def solution(mesh):
    return jax.shard_map(
        local,
        mesh=mesh,
        in_specs=(P(AXES, None), P(AXES), P(AXES), P()),
        out_specs=(P(AXES, None), P(AXES)),
        check_vma=False,
    )
```
